32 devices in a mesh: dp: 4 (over y, x), fsdp: 8 (over z, core).
Axes of the slice: x: 2, y: 2, z: 4, core: 2. Of those that a mesh axis runs over, the one named last changes fastest.
Arguments:
- input_tokens: int32 [2, 32768], P(None, ('dp', 'fsdp')), may hold values from 0 to 29
- item_numbers: int32 [2, 32768], P(None, ('dp', 'fsdp')), may hold values from -1 to 3, as said below
- loss_positions: int32 [2, 4096], P(None, ('dp', 'fsdp')), may hold values from -1 to 1023, as said below
- target_tokens: int32 [2, 4096], P(None, ('dp', 'fsdp')), may hold values from 0 to 29
- input_projection: float32 [1280, 640], P('fsdp', 'dp'), may hold values from -0.15625 to 0.15625
- dilated_conv: float32 [3200, 640], P('fsdp', 'dp'), may hold values from -0.109375 to 0.109375
- output_projection: float32 [1280, 640], P('fsdp', 'dp'), may hold values from -0.25 to 0.25
- vectors: float32 [68, 1280], P(None, ('dp', 'fsdp'))
- input_first_moment: float32 [1280, 640], P('fsdp'), may hold values from -6.67572e-06 to 6.67572e-06
- input_second_moment: float32 [1280, 640], P('fsdp'), may hold values from 5.3002034e-12 to 2.1200814e-11
- conv_first_moment: float32 [3200, 640], P('fsdp'), may hold values from -6.67572e-06 to 6.67572e-06
- conv_second_moment: float32 [3200, 640], P('fsdp'), may hold values from 5.3002034e-12 to 2.1200814e-11
- output_first_moment: float32 [1280, 640], P('fsdp'), may hold values from -6.67572e-06 to 6.67572e-06
- output_second_moment: float32 [1280, 640], P('fsdp'), may hold values from 5.3002034e-12 to 2.1200814e-11
- vector_first_moment: float32 [68, 1280], P(None, ('dp', 'fsdp')), may hold values from -1.9073486e-05 to 1.9073486e-05
- vector_second_moment: float32 [68, 1280], P(None, ('dp', 'fsdp')), may hold values from 4.7701832e-11 to 1.9080733e-10
- bases: float32 [3, 640, 640], replicated, as said below
- eigenbasis_flags: int32 [3], replicated, may hold values from 0 to 1, as said below
- optimizer_step: int32 [1], replicated, may hold values from 2 to 20
Outputs:
- mean_loss: float32 [], replicated
- grad_norm: float32 [], replicated
- master_in: float32 [1280, 640], P('fsdp', 'dp')
- copy_in: bfloat16 [1280, 640], P('fsdp', 'dp')
- moment_in: float32 [1280, 640], P('fsdp')
- square_in: float32 [1280, 640], P('fsdp')
- updated_conv: float32 [3200, 640], P('fsdp', 'dp')
- conv_bfloat_copy: bfloat16 [3200, 640], P('fsdp', 'dp')
- updated_conv_moment: float32 [3200, 640], P('fsdp')
- updated_conv_square: float32 [3200, 640], P('fsdp')
- master_out: float32 [1280, 640], P('fsdp', 'dp')
- copy_out: bfloat16 [1280, 640], P('fsdp', 'dp')
- moment_out: float32 [1280, 640], P('fsdp')
- square_out: float32 [1280, 640], P('fsdp')
- master_vec: float32 [68, 1280], P(None, ('dp', 'fsdp'))
- copy_vec: bfloat16 [68, 1280], P(None, ('dp', 'fsdp'))
- moment_vec: float32 [68, 1280], P(None, ('dp', 'fsdp'))
- square_vec: float32 [68, 1280], P(None, ('dp', 'fsdp'))
The draws below stay inside these ranges and needn't reach their ends.
Inputs may be any that keep to these rules, and one draw needn't show every extreme that they name: `item_numbers`: each device's 1024 slots of a micro-batch hold whole items of 256, 512 or 1024 tokens, numbered from 0 in order and starting at slot 0, followed by padding marked -1; items fill at least half of the slots; some device holds one item of 1024 tokens. `loss_positions`: slot i of a device's 128 slots in a micro-batch holds -1 or a position from 8 i to 8 i + 7 of that device's slots; it holds a position exactly when that position belongs to an item. `eigenbasis_flags`: two of the three entries are 1. `bases`: each matrix is orthogonal.
All inputs are finite; a program needn't handle non-finite values.
Results may differ from the reference program's by a relative error of at most 0.0091.
Values may be sent and summed in bfloat16 or wider, within the bound.
A program may use at most 256 MiB of HBM per device.

```python
import math
from functools import partial
import jax
import jax.numpy as jnp
import numpy as np
from jax import lax

D = 1280
INNER_WIDTH = 640
VOCAB = 30
CONV_TAPS = 5
DILATION = 8
MICRO_BATCHES = 2
BLOCK = 256
DEVICE_SLOTS = 1024
LOSS_SLOTS = 128
TOKEN_SLOTS = 32768
SLOTS = 4096
VROWS = 68
NPARAM = 3773440


layout_table = np.array([[0, 0, 0, 0], [0, 0, 1, 1], [0, 0, 1, 2], [0, 1, 2, 3], [0, 0, 1, -1], [0, 1, -1, -1], [0, 0, -1, -1], [0, 1, 2, -1]], dtype=np.int32)


def item_layout(key):
    buffer_list = TOKEN_SLOTS // DEVICE_SLOTS
    layout_ids = jnp.asarray(layout_table)
    layouts = jax.random.randint(jax.random.fold_in(key, 11), (MICRO_BATCHES, buffer_list), 0, 8)
    layouts = layouts.at[0, 0].set(0).at[0, 1].set(3).at[1, 0].set(5)
    chosen = layout_ids[layouts]
    block_of = jnp.arange(DEVICE_SLOTS, dtype=jnp.int32) // BLOCK
    item_matrix = chosen[:, :, block_of]
    live_tokens = jnp.sum((chosen >= 0).astype(jnp.int32), axis=-1) * BLOCK
    small_noise = jax.random.randint(jax.random.fold_in(key, 12), (MICRO_BATCHES, buffer_list, LOSS_SLOTS), 0, 8)
    small_noise = small_noise.at[0, 0, LOSS_SLOTS - 1].set(7)
    place_list = jnp.arange(LOSS_SLOTS, dtype=jnp.int32)[None, None, :] * 8 + small_noise
    slot_matrix = jnp.where(place_list < live_tokens[:, :, None], place_list, -1)
    return (item_matrix.reshape(MICRO_BATCHES, TOKEN_SLOTS).astype(jnp.int32), slot_matrix.reshape(MICRO_BATCHES, buffer_list * LOSS_SLOTS).astype(jnp.int32))


def draw_item_numbers(key, part):
    return item_layout(key)[0]


def draw_loss_positions(key, part):
    return item_layout(key)[1]


def draw_vectors(key, part):
    normal_vals = jax.random.normal(key, (VROWS, D), jnp.float32)
    uniform_vals = jax.random.uniform(jax.random.fold_in(key, 3), (VROWS, D), jnp.float32, 0.7, 1.3)
    row_pos = jnp.arange(VROWS, dtype=jnp.int32)[:, None]
    col_pos = jnp.arange(D, dtype=jnp.int32)[None, :]
    starting_row = 2 * VOCAB
    gain_mask = (row_pos == starting_row) | (row_pos == starting_row + 3) | ((row_pos == starting_row + 5) | (row_pos == starting_row + 7)) & (col_pos < INNER_WIDTH)
    row_scale = jnp.where(row_pos < VOCAB, 1.0, jnp.where(row_pos < starting_row, 2.0 / math.sqrt(D), 0.1))
    return jnp.where(gain_mask, uniform_vals, normal_vals * row_scale).astype(jnp.float32)


def draw_bases(key, part):
    low_bits = (INNER_WIDTH & -INNER_WIDTH).bit_length() - 1
    odd_part = INNER_WIDTH >> low_bits
    position = jnp.arange(INNER_WIDTH, dtype=jnp.int32)
    high_row = (position >> low_bits)[:, None]
    high_col = (position >> low_bits)[None, :]
    row_level = jnp.where(high_row == 0, math.sqrt(1.0 / odd_part), math.sqrt(2.0 / odd_part))
    cosine = jnp.cos(math.pi * (2 * high_col + 1).astype(jnp.float32) * high_row.astype(jnp.float32) / (2 * odd_part))
    sign_vals = (jax.random.randint(jax.random.fold_in(key, 5), (3, odd_part), 0, 2) * 2 - 1).astype(jnp.float32)
    result = sign_vals[:, position >> low_bits][:, :, None] * (row_level * cosine)[None]
    angles = jax.random.uniform(key, (3, max(low_bits, 1)), jnp.float32, -math.pi, math.pi)
    for bit_index in range(low_bits):
        row_bit = (position >> bit_index & 1)[:, None]
        col_bit = (position >> bit_index & 1)[None, :]
        cos_part = jnp.cos(angles[:, bit_index])[:, None, None]
        sin_part = jnp.sin(angles[:, bit_index])[:, None, None]
        factor = jnp.where(row_bit == col_bit, cos_part, jnp.where(row_bit == 1, sin_part, -sin_part))
        result = result * factor
    return result.astype(jnp.float32)


def draw_eigenbasis_flags(key, part):
    shuffled = jax.random.permutation(key, 3)
    return (shuffled < 2).astype(jnp.int32)


def with_ends(values, rng, least, high):
    longest = values.shape.index(max(values.shape))
    spots = []
    for shift in (0, 1):
        where = [jax.random.randint(jax.random.fold_in(rng, axis), (), 0, length) for axis, length in enumerate(values.shape)]
        where[longest] = (where[longest] + shift) % values.shape[longest]
        spots.append(tuple(where))
    return values.at[spots[0]].set(least).at[spots[1]].set(high)


def steps_of(key, extent, shards, smallest, high):
    def one(axis_at, blocks):
        heights = jax.random.uniform(jax.random.fold_in(jax.random.fold_in(key, 6), axis_at), (blocks,), jnp.float32, smallest / len(shards), high / len(shards))
        return jnp.repeat(jnp.exp(heights), extent[axis_at] // blocks).reshape((-1,) + (1,) * (len(extent) - axis_at - 1))

    loudness = one(*shards[0])
    for cut in shards[1:]:
        loudness = loudness * one(*cut)
    return loudness


def bell_draw(key, shape, scale, bound, pieces=(), kind=jnp.bfloat16):
    gain = steps_of(key, shape, pieces, -0.22, 0.18) if pieces else 1.0
    drawn = jax.random.normal(key, shape, jnp.float32) * scale * gain
    return jnp.minimum(jnp.maximum(drawn, -bound), bound).astype(kind)


def setup_inputs(seed: int = 0) -> dict:
    streams_of = jax.random.split(jax.random.key(seed), 20)
    return {
        "input_tokens": with_ends(jax.random.randint(streams_of[0], (MICRO_BATCHES, TOKEN_SLOTS), 0, VOCAB), jax.random.fold_in(streams_of[0], 1), 0, VOCAB - 1).astype(jnp.int32),
        "item_numbers": draw_item_numbers(jax.random.fold_in(streams_of[19], 71), 0),
        "loss_positions": draw_loss_positions(jax.random.fold_in(streams_of[19], 71), 0),
        "target_tokens": with_ends(jax.random.randint(streams_of[3], (MICRO_BATCHES, SLOTS), 0, VOCAB), jax.random.fold_in(streams_of[3], 1), 0, VOCAB - 1).astype(jnp.int32),
        "input_projection": bell_draw(streams_of[4], (D, INNER_WIDTH), D ** -0.5, 0.15625, ((0, 8), (1, 4)), jnp.float32),
        "dilated_conv": bell_draw(streams_of[5], (CONV_TAPS * INNER_WIDTH, INNER_WIDTH), (CONV_TAPS * INNER_WIDTH) ** -0.5, 0.109375, ((0, 8), (1, 4)), jnp.float32),
        "output_projection": bell_draw(streams_of[6], (D, INNER_WIDTH), INNER_WIDTH ** -0.5, 0.25, ((0, 8), (1, 4)), jnp.float32),
        "vectors": draw_vectors(jax.random.fold_in(streams_of[19], 71), 0),
        "input_first_moment": bell_draw(streams_of[8], (D, INNER_WIDTH), (0.0022 * NPARAM ** -0.5), 6.67572021484375e-06, ((0, 8),), jnp.float32),
        "input_second_moment": jnp.clip(jnp.exp(math.log(2.120081367407156e-11) - 1.3862944 * jax.random.uniform(streams_of[9], (D, INNER_WIDTH), jnp.float32) ** steps_of(streams_of[9], (D, INNER_WIDTH), ((0, 8),), -0.2, 0.2)), 5.30020341851789e-12, 2.120081367407156e-11),
        "conv_first_moment": bell_draw(streams_of[10], (CONV_TAPS * INNER_WIDTH, INNER_WIDTH), (0.0022 * NPARAM ** -0.5), 6.67572021484375e-06, ((0, 8),), jnp.float32),
        "conv_second_moment": jnp.clip(jnp.exp(math.log(2.120081367407156e-11) - 1.3862944 * jax.random.uniform(streams_of[11], (CONV_TAPS * INNER_WIDTH, INNER_WIDTH), jnp.float32) ** steps_of(streams_of[11], (CONV_TAPS * INNER_WIDTH, INNER_WIDTH), ((0, 8),), -0.2, 0.2)), 5.30020341851789e-12, 2.120081367407156e-11),
        "output_first_moment": bell_draw(streams_of[12], (D, INNER_WIDTH), (0.0022 * NPARAM ** -0.5), 6.67572021484375e-06, ((0, 8),), jnp.float32),
        "output_second_moment": jnp.clip(jnp.exp(math.log(2.120081367407156e-11) - 1.3862944 * jax.random.uniform(streams_of[13], (D, INNER_WIDTH), jnp.float32) ** steps_of(streams_of[13], (D, INNER_WIDTH), ((0, 8),), -0.2, 0.2)), 5.30020341851789e-12, 2.120081367407156e-11),
        "vector_first_moment": bell_draw(streams_of[14], (VROWS, D), (0.0066 * NPARAM ** -0.5), 1.9073486328125e-05, ((1, 32),), jnp.float32),
        "vector_second_moment": jnp.clip(jnp.exp(math.log(1.9080732827081448e-10) - 1.3862944 * jax.random.uniform(streams_of[15], (VROWS, D), jnp.float32) ** steps_of(streams_of[15], (VROWS, D), ((1, 32),), -0.2, 0.2)), 4.770183206770362e-11, 1.9080732827081448e-10),
        "bases": draw_bases(jax.random.fold_in(streams_of[19], 71), 0),
        "eigenbasis_flags": draw_eigenbasis_flags(jax.random.fold_in(streams_of[19], 71), 0),
        "optimizer_step": jax.random.randint(streams_of[18], (1,), 2, 21).astype(jnp.int32),
    }


@jax.custom_vjp
def lower_precision(v):
    return lax.optimization_barrier(v.astype(jnp.bfloat16)).astype(jnp.float32)

@jax.custom_vjp
def lower_backward(v):
    return v

def low_keep(v):
    return (lower_precision(v), None)

def low_pass(kept, grad):
    return (grad,)

def back_keep(v):
    return (v, None)

def back_low(kept, grad):
    return (lower_precision(grad),)
lower_precision.defvjp(low_keep, low_pass)
lower_backward.defvjp(back_keep, back_low)
beta_one = 0.9
beta_two = 0.95
epsilon = 1e-08
rate_matrix = 0.02
rate_vector = 0.5
decay_weight = 0.01
clip_limit = 0.02
norm_eps = 1e-05
highest_precision = lax.Precision.HIGHEST

def layer_norm(values, norm_gain, norm_bias):
    centre = values - lax.optimization_barrier(jnp.mean(values, axis=-1, keepdims=True))
    spread = lax.optimization_barrier(jnp.mean(centre * centre, axis=-1, keepdims=True))
    return centre * lax.rsqrt(spread + norm_eps) * norm_gain + norm_bias

def norm_gelu(values, norm_gain, norm_bias):
    return jax.nn.gelu(layer_norm(values, norm_gain, norm_bias), approximate=True)

def shifted(values, offset, filler):
    if offset > 0:
        pad_rows = jnp.full((offset,) + values.shape[1:], filler, values.dtype)
        return jnp.concatenate([values[offset:], pad_rows], axis=0)
    if offset < 0:
        pad_rows = jnp.full((-offset,) + values.shape[1:], filler, values.dtype)
        return jnp.concatenate([pad_rows, values[:offset]], axis=0)
    return values

def build_masks(item_row):
    result = []
    for tap_index in range(CONV_TAPS):
        offset = (tap_index - CONV_TAPS // 2) * DILATION
        same_item = (shifted(item_row, offset, -2) == item_row) & (item_row >= 0)
        result.append((offset, same_item))
    return result

def unfold(values, masks):
    return jnp.concatenate([shifted(values, offset, 0) * same_item[:, None].astype(values.dtype) for offset, same_item in masks], axis=1)

def slot_loss(logits, labels, valid_slot):
    log_total = jax.nn.logsumexp(logits, axis=-1)
    hits = labels[:, None] == jnp.arange(logits.shape[1], dtype=jnp.int32)[None, :]
    chosen = lax.optimization_barrier(jnp.sum(jnp.where(hits, logits, 0.0), axis=-1))
    return jnp.sum(jnp.where(valid_slot, log_total - chosen, 0.0))

def buffer_loss(parameter_list, tokens, item_row, slot_list, targets):
    input_projection, dilated_conv, output_projection, embedding_table = parameter_list
    starting_row = 2 * VOCAB
    embedded = embedding_table[:VOCAB][tokens]
    first_act = lower_precision(norm_gelu(embedded, embedding_table[starting_row], embedding_table[starting_row + 1]))
    pre_inner = lower_backward(jnp.dot(first_act, input_projection, precision=highest_precision) + embedding_table[starting_row + 6, :INNER_WIDTH])
    second_act = lower_precision(norm_gelu(pre_inner, embedding_table[starting_row + 5, :INNER_WIDTH], embedding_table[starting_row + 5, INNER_WIDTH:]))
    column_list = unfold(second_act, build_masks(item_row))
    conv_input = lower_backward(jnp.dot(column_list, dilated_conv, precision=highest_precision) + embedding_table[starting_row + 6, INNER_WIDTH:])
    third_act = lower_precision(norm_gelu(conv_input, embedding_table[starting_row + 7, :INNER_WIDTH], embedding_table[starting_row + 7, INNER_WIDTH:]))
    branch = lower_backward(jnp.dot(third_act, output_projection.T, precision=highest_precision) + embedding_table[starting_row + 2])
    final_out = layer_norm(embedded + branch, embedding_table[starting_row + 3], embedding_table[starting_row + 4])
    picked = lower_precision(final_out[jnp.maximum(slot_list, 0)])
    logits = lower_backward(jnp.dot(picked, embedding_table[VOCAB:starting_row].T, precision=highest_precision))
    return slot_loss(logits, targets, slot_list >= 0)

def overall_loss(input_projection, dilated_conv, output_projection, vectors, input_tokens, item_numbers, loss_positions, target_tokens):
    parameter_list = (lower_precision(input_projection), lower_precision(dilated_conv), lower_precision(output_projection), lower_precision(vectors))

    def buffer_function(inputs):
        return buffer_loss(parameter_list, inputs[0], inputs[1], inputs[2], inputs[3])
    buffer_entries = lax.map(jax.checkpoint(buffer_function), (input_tokens.reshape(-1, DEVICE_SLOTS), item_numbers.reshape(-1, DEVICE_SLOTS), loss_positions.reshape(-1, LOSS_SLOTS), target_tokens.reshape(-1, LOSS_SLOTS)))
    return jnp.sum(buffer_entries)

def eigenbasis_update(gradient, master, moment, square, rotated_grads, first_correction, second_correction):
    rotated = jnp.dot(gradient, rotated_grads, precision=highest_precision)
    moment_new = beta_one * moment + (1.0 - beta_one) * rotated
    square_new = beta_two * square + (1.0 - beta_two) * rotated * rotated
    step_ratio = moment_new / first_correction / (jnp.sqrt(square_new / second_correction) + epsilon)
    update = jnp.dot(step_ratio, rotated_grads.T, precision=highest_precision)
    master_new = master - rate_matrix * (update + decay_weight * master)
    return (master_new, master_new.astype(jnp.bfloat16), moment_new, square_new)

def adam_vectors(gradient, master, moment, square, first_correction, second_correction):
    decay_rows = jnp.where(jnp.arange(master.shape[0], dtype=jnp.int32)[:, None] < 2 * VOCAB, decay_weight, 0.0)
    moment_new = beta_one * moment + (1.0 - beta_one) * gradient
    square_new = beta_two * square + (1.0 - beta_two) * gradient * gradient
    step_ratio = moment_new / first_correction / (jnp.sqrt(square_new / second_correction) + epsilon)
    master_new = master - rate_vector * (step_ratio + decay_rows * master)
    return (master_new, master_new.astype(jnp.bfloat16), moment_new, square_new)

def reference(input_tokens, item_numbers, loss_positions, target_tokens, input_projection, dilated_conv, output_projection, vectors, input_first_moment, input_second_moment, conv_first_moment, conv_second_moment, output_first_moment, output_second_moment, vector_first_moment, vector_second_moment, bases, eigenbasis_flags, optimizer_step):
    loss_function = partial(overall_loss, input_tokens=input_tokens, item_numbers=item_numbers, loss_positions=loss_positions, target_tokens=target_tokens)
    summed_loss, backward_function = jax.vjp(loss_function, input_projection, dilated_conv, output_projection, vectors)
    gradients = backward_function(jnp.ones_like(summed_loss))
    slot_count = jnp.sum((loss_positions >= 0).astype(jnp.float32))
    square_sum = sum((jnp.sum(gradient * gradient) for gradient in gradients))
    grad_norm = jnp.sqrt(square_sum) / slot_count
    factor = jnp.minimum(1.0, clip_limit / grad_norm) / slot_count
    clipped_grads = [gradient * factor for gradient in gradients]
    step_value = optimizer_step[0].astype(jnp.float32)
    first_correction = 1.0 - beta_one ** step_value
    second_correction = 1.0 - beta_two ** step_value
    identity = jnp.eye(INNER_WIDTH, dtype=jnp.float32)
    rotated_grads = [jnp.where(eigenbasis_flags[mat_index] == 1, bases[mat_index], identity) for mat_index in range(3)]
    master_in, copy_in, moment_in, square_in = eigenbasis_update(clipped_grads[0], input_projection, input_first_moment, input_second_moment, rotated_grads[0], first_correction, second_correction)
    updated_conv, conv_bfloat_copy, updated_conv_moment, updated_conv_square = eigenbasis_update(clipped_grads[1], dilated_conv, conv_first_moment, conv_second_moment, rotated_grads[1], first_correction, second_correction)
    master_out, copy_out, moment_out, square_out = eigenbasis_update(clipped_grads[2], output_projection, output_first_moment, output_second_moment, rotated_grads[2], first_correction, second_correction)
    master_vec, copy_vec, moment_vec, square_vec = adam_vectors(clipped_grads[3], vectors, vector_first_moment, vector_second_moment, first_correction, second_correction)
    return (summed_loss / slot_count, grad_norm, master_in, copy_in, moment_in, square_in, updated_conv, conv_bfloat_copy, updated_conv_moment, updated_conv_square, master_out, copy_out, moment_out, square_out, master_vec, copy_vec, moment_vec, square_vec)
```

```python
from functools import partial

import jax
import jax.numpy as jnp
from jax import lax
from jax.sharding import PartitionSpec as P

VOCAB = 30
CONV_TAPS = 5
DILATION = 8
TABLE = 32


beta_one = 0.9
beta_two = 0.95
epsilon = 1e-08
rate_matrix = 0.02
rate_vector = 0.5
decay_weight = 0.01
clip_limit = 0.02
norm_eps = 1e-05
highest_precision = lax.Precision.HIGHEST


def layer_norm(values, norm_gain, norm_bias):
    centre = values - jnp.mean(values, axis=-1, keepdims=True)
    spread = jnp.mean(centre * centre, axis=-1, keepdims=True)
    return centre * lax.rsqrt(spread + norm_eps) * norm_gain + norm_bias


def norm_gelu(values, norm_gain, norm_bias):
    return jax.nn.gelu(layer_norm(values, norm_gain, norm_bias), approximate=True)


def slot_loss(logits, labels, valid_slot):
    log_total = jax.nn.logsumexp(logits, axis=-1)
    hits = labels[:, None] == jnp.arange(logits.shape[1], dtype=jnp.int32)[None, :]
    chosen = jnp.sum(jnp.where(hits, logits, 0.0), axis=-1)
    return jnp.sum(jnp.where(valid_slot, log_total - chosen, 0.0))


def moved_groups(values, step):
    if step > 0:
        return jnp.concatenate([values[:, step:], jnp.full_like(values[:, :step], -1)], axis=1)
    if step < 0:
        return jnp.concatenate([jnp.full_like(values[:, :-step], -1), values[:, :step]], axis=1)
    return values


def tap_onehots(tokens, items, positions):
    batches, slots = positions.shape
    stride = tokens.shape[1] // slots
    token_groups = tokens.reshape(batches, slots, stride)
    item_groups = items.reshape(batches, slots, stride)
    valid = positions >= 0
    residue = jnp.where(valid, positions - stride * jnp.arange(slots, dtype=jnp.int32)[None], -1)
    chosen = residue[:, :, None] == jnp.arange(stride, dtype=jnp.int32)[None, None]
    own_item = jnp.sum(jnp.where(chosen, item_groups, 0), axis=2)
    identities = jnp.arange(TABLE, dtype=jnp.int32)
    result = []
    for tap in range(CONV_TAPS):
        step = (tap - CONV_TAPS // 2) * DILATION // stride
        item = jnp.sum(jnp.where(chosen, moved_groups(item_groups, step), 0), axis=2)
        token = jnp.sum(jnp.where(chosen, moved_groups(token_groups, step), 0), axis=2)
        keep = valid & (item == own_item) & (own_item >= 0)
        result.append(jnp.where(keep, token, -1)[:, :, None] == identities)
    return jnp.concatenate(result, axis=2).reshape(batches * slots, CONV_TAPS * TABLE)


def exact_dot(left, right, contract):
    high = left.astype(jnp.bfloat16)
    low = (left - high.astype(jnp.float32)).astype(jnp.bfloat16)
    return lax.dot_general(high, right, contract, preferred_element_type=jnp.float32) + lax.dot_general(
        low, right, contract, preferred_element_type=jnp.float32
    )


def column_sum(values):
    return jnp.sum(values, axis=0, dtype=jnp.float32)


def gathered_weights(shards):
    parted = (
        lax.all_gather(shards[0], "fsdp", axis=0, tiled=True),
        lax.all_gather(shards[1], "fsdp", axis=0, tiled=True),
        lax.all_gather(shards[2], "fsdp", axis=0, tiled=True),
        lax.all_gather(shards[3], "fsdp", axis=1, tiled=True),
    )
    return (
        lax.all_gather(parted[0], "dp", axis=1, tiled=True),
        lax.all_gather(parted[1], "dp", axis=1, tiled=True),
        lax.all_gather(parted[2], "dp", axis=1, tiled=True),
        lax.all_gather(parted[3], "dp", axis=1, tiled=True),
    )


def eigenbasis_update(
    gradient, master, moment, square, rotated_grads, col_start, first_correction, second_correction
):
    rotated = jnp.dot(gradient, rotated_grads, precision=highest_precision)
    moment_new = beta_one * moment + (1.0 - beta_one) * rotated
    square_new = beta_two * square + (1.0 - beta_two) * rotated * rotated
    step_ratio = (
        moment_new / first_correction / (jnp.sqrt(square_new / second_correction) + epsilon)
    )
    own_basis = lax.dynamic_slice_in_dim(rotated_grads, col_start, master.shape[1], 0)
    update = jnp.einsum("ri,ci->rc", step_ratio, own_basis, precision=highest_precision)
    master_new = master - rate_matrix * (update + decay_weight * master)
    return (master_new, master_new.astype(jnp.bfloat16), moment_new, square_new)


def adam_vectors(gradient, master, moment, square, first_correction, second_correction):
    decay_rows = jnp.where(
        jnp.arange(master.shape[0], dtype=jnp.int32)[:, None] < 2 * VOCAB, decay_weight, 0.0
    )
    moment_new = beta_one * moment + (1.0 - beta_one) * gradient
    square_new = beta_two * square + (1.0 - beta_two) * gradient * gradient
    step_ratio = (
        moment_new / first_correction / (jnp.sqrt(square_new / second_correction) + epsilon)
    )
    master_new = master - rate_vector * (step_ratio + decay_rows * master)
    return (master_new, master_new.astype(jnp.bfloat16), moment_new, square_new)


def local(
    input_tokens,
    item_numbers,
    loss_positions,
    target_tokens,
    input_projection,
    dilated_conv,
    output_projection,
    vectors,
    input_first_moment,
    input_second_moment,
    conv_first_moment,
    conv_second_moment,
    output_first_moment,
    output_second_moment,
    vector_first_moment,
    vector_second_moment,
    bases,
    eigenbasis_flags,
    optimizer_step,
):
    shards_low = (
        input_projection.astype(jnp.bfloat16),
        dilated_conv.astype(jnp.bfloat16),
        output_projection.astype(jnp.bfloat16),
        vectors.astype(jnp.bfloat16),
    )
    weight_in, weight_conv, weight_out, table_low = gathered_weights(shards_low)
    groups, col_index = lax.axis_size("dp"), lax.axis_index("dp")
    rows, row_index = lax.axis_size("fsdp"), lax.axis_index("fsdp")
    inner = weight_in.shape[1]
    width = weight_in.shape[0]
    start = 2 * VOCAB
    table = table_low.astype(jnp.float32)
    head = table_low[VOCAB:start]
    onehots = tap_onehots(input_tokens, item_numbers, loss_positions)
    onehots_low = onehots.astype(jnp.bfloat16)
    centre = CONV_TAPS // 2 * TABLE
    centre_low = onehots_low[:, centre : centre + TABLE]
    embedded = jnp.concatenate([table_low[:VOCAB], jnp.zeros((TABLE - VOCAB, width), jnp.bfloat16)], axis=0)
    first_act, first_back = jax.vjp(
        norm_gelu, embedded.astype(jnp.float32), table[start], table[start + 1]
    )
    first_low = first_act.astype(jnp.bfloat16)
    pre_inner = (
        jnp.dot(first_low, weight_in, preferred_element_type=jnp.float32)
        + table[start + 6, :inner]
    )
    second_act, second_back = jax.vjp(
        norm_gelu, pre_inner, table[start + 5, :inner], table[start + 5, inner:]
    )
    second_low = second_act.astype(jnp.bfloat16)
    picked_act = [
        jnp.dot(
            onehots_low[:, tap * TABLE : (tap + 1) * TABLE],
            second_low,
            preferred_element_type=jnp.float32,
        ).astype(jnp.bfloat16)
        for tap in range(CONV_TAPS)
    ]
    conv_input = (
        jnp.dot(
            jnp.concatenate(picked_act, axis=1), weight_conv, preferred_element_type=jnp.float32
        )
        + table[start + 6, inner:]
    )
    third_act, third_back = jax.vjp(
        norm_gelu, conv_input, table[start + 7, :inner], table[start + 7, inner:]
    )
    third_low = third_act.astype(jnp.bfloat16)
    branch = (
        jnp.einsum("ti,di->td", third_low, weight_out, preferred_element_type=jnp.float32)
        + table[start + 2]
    )
    picked_embedded = jnp.dot(centre_low, embedded, preferred_element_type=jnp.float32)
    final_out, final_back = jax.vjp(
        layer_norm, picked_embedded + branch, table[start + 3], table[start + 4]
    )
    picked = final_out.astype(jnp.bfloat16)
    logits = jnp.einsum("pd,vd->pv", picked, head, preferred_element_type=jnp.float32)
    valid = loss_positions.reshape(-1) >= 0
    summed_loss, loss_back = jax.vjp(
        partial(slot_loss, labels=target_tokens.reshape(-1), valid_slot=valid), logits
    )
    logit_grad = loss_back(jnp.ones((), jnp.float32))[0].astype(jnp.bfloat16)
    head_grad = jnp.einsum("pv,pd->vd", logit_grad, picked, preferred_element_type=jnp.float32)
    picked_grad = jnp.dot(logit_grad, head, preferred_element_type=jnp.float32)
    sum_grad, gain_four, bias_four = final_back(picked_grad)
    branch_low = sum_grad.astype(jnp.bfloat16)
    out_grad = jnp.einsum("td,ti->di", branch_low, third_low, preferred_element_type=jnp.float32)
    third_grad = jnp.dot(branch_low, weight_out, preferred_element_type=jnp.float32)
    conv_pre, gain_three, bias_three = third_back(third_grad)
    conv_low = conv_pre.astype(jnp.bfloat16)
    tap_grads = lax.dot_general(
        onehots_low, conv_low, (((0,), (0,)), ((), ())), preferred_element_type=jnp.float32
    )
    start_grads = jnp.einsum(
        "tv,td->vd", centre_low.astype(jnp.float32), sum_grad, precision=highest_precision
    )
    slot_count = jnp.sum(valid.astype(jnp.float32))
    wide_rows = jnp.concatenate(
        [
            start_grads[:VOCAB],
            head_grad,
            jnp.stack(
                [
                    column_sum(branch_low),
                    gain_four,
                    bias_four,
                    jnp.concatenate([gain_three, bias_three]),
                ]
            ),
        ],
        axis=0,
    )
    out_rows = lax.psum(
        lax.psum_scatter(out_grad.astype(jnp.bfloat16), "fsdp", scatter_dimension=0, tiled=True), "dp"
    ).astype(jnp.float32)
    tap_grads, wide_rows, summed_loss, slot_count = lax.psum(
        (tap_grads, wide_rows, summed_loss, slot_count), ("dp", "fsdp")
    )

    tap_view = tap_grads.reshape(CONV_TAPS, TABLE, inner)
    second_grad = sum(
        exact_dot(tap_view[tap], weight_conv[tap * inner : (tap + 1) * inner], (((1,), (1,)), ((), ())))
        for tap in range(CONV_TAPS)
    )
    inner_pre, gain_two, bias_two = second_back(second_grad)
    first_grad = exact_dot(inner_pre, weight_in, (((1,), (1,)), ((), ())))
    table_grad, gain_one, bias_one = first_back(first_grad)
    vec_sum = jnp.concatenate(
        [
            table_grad[:VOCAB] + wide_rows[:VOCAB],
            wide_rows[VOCAB:start],
            jnp.stack(
                [
                    gain_one,
                    bias_one,
                    wide_rows[start],
                    wide_rows[start + 1],
                    wide_rows[start + 2],
                    jnp.concatenate([gain_two, bias_two]),
                    jnp.concatenate(
                        [jnp.sum(inner_pre, axis=0), jnp.sum(tap_view[CONV_TAPS // 2], axis=0)]
                    ),
                    wide_rows[start + 3],
                ]
            ),
        ],
        axis=0,
    )
    own = width // (groups * rows)
    vec_own = lax.dynamic_slice_in_dim(vec_sum, (col_index * rows + row_index) * own, own, 1)

    row_low = lax.dynamic_slice_in_dim(first_low, row_index * (width // rows), width // rows, 1)
    in_rows = jnp.einsum(
        "vr,vi->ri", row_low.astype(jnp.float32), inner_pre, precision=highest_precision
    )
    placed = (
        jnp.eye(CONV_TAPS, dtype=jnp.bfloat16)[:, None, :, None] * second_low[None, :, None, :]
    ).reshape(CONV_TAPS * TABLE, CONV_TAPS * inner)
    conv_count = CONV_TAPS * inner // rows
    conv_low_rows = lax.dynamic_slice_in_dim(placed, row_index * conv_count, conv_count, 1)
    conv_rows = jnp.einsum(
        "vr,vi->ri", conv_low_rows.astype(jnp.float32), tap_grads, precision=highest_precision
    )

    col_width = input_projection.shape[1]
    col_start = col_index * col_width
    owned = [
        lax.dynamic_slice_in_dim(full_rows, col_start, col_width, 1)
        for full_rows in (in_rows, conv_rows, out_rows)
    ]
    square_local = sum((jnp.sum(piece * piece) for piece in owned)) + jnp.sum(vec_own * vec_own)
    square_total = lax.psum(square_local, ("dp", "fsdp"))
    grad_norm = jnp.sqrt(square_total) / slot_count
    factor = jnp.minimum(1.0, clip_limit / grad_norm) / slot_count
    step_value = optimizer_step[0].astype(jnp.float32)
    first_correction = 1.0 - beta_one**step_value
    second_correction = 1.0 - beta_two**step_value
    identity = jnp.eye(bases.shape[1], dtype=jnp.float32)
    rotated_grads = [
        jnp.where(eigenbasis_flags[mat_index] == 1, bases[mat_index], identity)
        for mat_index in range(3)
    ]
    master_in, copy_in, moment_in, square_in = eigenbasis_update(
        in_rows * factor,
        input_projection,
        input_first_moment,
        input_second_moment,
        rotated_grads[0],
        col_start,
        first_correction,
        second_correction,
    )
    updated_conv, conv_bfloat_copy, updated_conv_moment, updated_conv_square = eigenbasis_update(
        conv_rows * factor,
        dilated_conv,
        conv_first_moment,
        conv_second_moment,
        rotated_grads[1],
        col_start,
        first_correction,
        second_correction,
    )
    master_out, copy_out, moment_out, square_out = eigenbasis_update(
        out_rows * factor,
        output_projection,
        output_first_moment,
        output_second_moment,
        rotated_grads[2],
        col_start,
        first_correction,
        second_correction,
    )
    master_vec, copy_vec, moment_vec, square_vec = adam_vectors(
        vec_own * factor,
        vectors,
        vector_first_moment,
        vector_second_moment,
        first_correction,
        second_correction,
    )
    return (
        summed_loss / slot_count,
        grad_norm,
        master_in,
        copy_in,
        moment_in,
        square_in,
        updated_conv,
        conv_bfloat_copy,
        updated_conv_moment,
        updated_conv_square,
        master_out,
        copy_out,
        moment_out,
        square_out,
        master_vec,
        copy_vec,
        moment_vec,
        square_vec,
    )


def solution(mesh):
    placed = (
        P(None, ("dp", "fsdp")),
        P(None, ("dp", "fsdp")),
        P(None, ("dp", "fsdp")),
        P(None, ("dp", "fsdp")),
        P("fsdp", "dp"),
        P("fsdp", "dp"),
        P("fsdp", "dp"),
        P(None, ("dp", "fsdp")),
        P("fsdp", None),
        P("fsdp", None),
        P("fsdp", None),
        P("fsdp", None),
        P("fsdp", None),
        P("fsdp", None),
        P(None, ("dp", "fsdp")),
        P(None, ("dp", "fsdp")),
        P(),
        P(),
        P(),
    )
    return jax.shard_map(
        local,
        mesh=mesh,
        in_specs=placed,
        out_specs=(
            P(),
            P(),
            P("fsdp", "dp"),
            P("fsdp", "dp"),
            P("fsdp", None),
            P("fsdp", None),
            P("fsdp", "dp"),
            P("fsdp", "dp"),
            P("fsdp", None),
            P("fsdp", None),
            P("fsdp", "dp"),
            P("fsdp", "dp"),
            P("fsdp", None),
            P("fsdp", None),
            P(None, ("dp", "fsdp")),
            P(None, ("dp", "fsdp")),
            P(None, ("dp", "fsdp")),
            P(None, ("dp", "fsdp")),
        ),
        check_vma=False,
    )
```

```python
from functools import partial

import jax
import jax.numpy as jnp
from jax import lax
from jax.experimental import pallas as pl
from jax.experimental.pallas import tpu as pltpu
from jax.sharding import PartitionSpec as P

VOCAB = 30
CONV_TAPS = 5
DILATION = 8
TABLE = 32
MESH = pl.DeviceIdType.MESH


beta_one = 0.9
beta_two = 0.95
epsilon = 1e-08
rate_matrix = 0.02
rate_vector = 0.5
decay_weight = 0.01
clip_limit = 0.02
norm_eps = 1e-05
highest_precision = lax.Precision.HIGHEST


def layer_norm(values, norm_gain, norm_bias):
    centre = values - jnp.mean(values, axis=-1, keepdims=True)
    spread = jnp.mean(centre * centre, axis=-1, keepdims=True)
    return centre * lax.rsqrt(spread + norm_eps) * norm_gain + norm_bias


def norm_gelu(values, norm_gain, norm_bias):
    return jax.nn.gelu(layer_norm(values, norm_gain, norm_bias), approximate=True)


def slot_loss(logits, labels, valid_slot):
    log_total = jax.nn.logsumexp(logits, axis=-1)
    hits = labels[:, None] == jnp.arange(logits.shape[1], dtype=jnp.int32)[None, :]
    chosen = jnp.sum(jnp.where(hits, logits, 0.0), axis=-1)
    return jnp.sum(jnp.where(valid_slot, log_total - chosen, 0.0))


def moved_groups(values, step):
    if step > 0:
        return jnp.concatenate([values[:, step:], jnp.full_like(values[:, :step], -1)], axis=1)
    if step < 0:
        return jnp.concatenate([jnp.full_like(values[:, :-step], -1), values[:, :step]], axis=1)
    return values


def tap_onehots(tokens, items, positions):
    batches, slots = positions.shape
    stride = tokens.shape[1] // slots
    token_groups = tokens.reshape(batches, slots, stride)
    item_groups = items.reshape(batches, slots, stride)
    valid = positions >= 0
    residue = jnp.where(valid, positions - stride * jnp.arange(slots, dtype=jnp.int32)[None], -1)
    chosen = residue[:, :, None] == jnp.arange(stride, dtype=jnp.int32)[None, None]
    own_item = jnp.sum(jnp.where(chosen, item_groups, 0), axis=2)
    identities = jnp.arange(TABLE, dtype=jnp.int32)
    result = []
    for tap in range(CONV_TAPS):
        step = (tap - CONV_TAPS // 2) * DILATION // stride
        item = jnp.sum(jnp.where(chosen, moved_groups(item_groups, step), 0), axis=2)
        token = jnp.sum(jnp.where(chosen, moved_groups(token_groups, step), 0), axis=2)
        keep = valid & (item == own_item) & (own_item >= 0)
        result.append(jnp.where(keep, token, -1)[:, :, None] == identities)
    return jnp.concatenate(result, axis=2).reshape(batches * slots, CONV_TAPS * TABLE)


def exact_dot(left, right, contract):
    high = left.astype(jnp.bfloat16)
    low = (left - high.astype(jnp.float32)).astype(jnp.bfloat16)
    return lax.dot_general(high, right, contract, preferred_element_type=jnp.float32) + lax.dot_general(
        low, right, contract, preferred_element_type=jnp.float32
    )


def column_sum(values):
    return jnp.sum(values, axis=0, dtype=jnp.float32)


def split_two(count):
    high = int(count**0.5)
    while count % high:
        high -= 1
    return high, count // high


def spread_peers(dp_size, fsdp_size):
    high, low = split_two(dp_size)
    depth = fsdp_size // 2
    me_dp, me_fsdp = lax.axis_index("dp"), lax.axis_index("fsdp")
    z, core = me_fsdp // 2, lax.rem(me_fsdp, 2)
    y, x = me_dp // low, lax.rem(me_dp, low)
    along_z = [lax.rem(z + i, depth) for i in range(1, depth)]
    along_y = [lax.rem(y + i, high) for i in range(1, high)]
    along_x = [lax.rem(x + i, low) for i in range(1, low)]
    return (z, y, x, core, low, along_z, along_y, along_x)


def meet(peers):
    barrier = pltpu.get_barrier_semaphore()
    for peer in peers:
        pl.semaphore_signal(barrier, inc=1, device_id=peer, device_id_type=MESH)
    pl.semaphore_wait(barrier, len(peers))


def gather_kernel(
    dp_size, fsdp_size, cut, shard_ref, vec_ref, out_ref, vec_out_ref, send_sem, recv_sem, own_sem
):
    z, y, x, core, low, along_z, along_y, along_x = spread_peers(dp_size, fsdp_size)
    me_dp, me_fsdp = y * low + x, z * 2 + core
    z_ids = [(me_dp, other * 2 + core) for other in along_z]
    y_ids = [(other * low + x, me_fsdp) for other in along_y]
    x_ids = [(y * low + other, me_fsdp) for other in along_x]
    partner = (me_dp, z * 2 + 1 - core)
    meet(z_ids + y_ids + x_ids + [partner])
    parts = ((0, cut), (cut, shard_ref.shape[0] - cut))

    def place(piece, column, row):
        if piece == 0:
            return vec_out_ref.at[column, row]
        begin, size = parts[piece - 1]
        return out_ref.at[row, column, pl.ds(begin, size)]

    def source(piece):
        if piece == 0:
            return vec_ref
        begin, size = parts[piece - 1]
        return shard_ref.at[pl.ds(begin, size)]

    started = []

    def push(piece, column, row, held, peers):
        for peer in peers:
            copy = pltpu.make_async_remote_copy(
                src_ref=held,
                dst_ref=place(piece, column, row),
                send_sem=send_sem.at[len(started)],
                recv_sem=recv_sem.at[piece, column, row],
                device_id=peer,
                device_id_type=MESH,
            )
            copy.start()
            started.append(copy)

    def arrived(piece, column, row):
        block = place(piece, column, row)
        pltpu.make_async_remote_copy(
            src_ref=block,
            dst_ref=block,
            send_sem=send_sem.at[0],
            recv_sem=recv_sem.at[piece, column, row],
            device_id=partner,
            device_id_type=MESH,
        ).wait_recv()
        return block

    def dims(piece):
        if piece == 2:
            return (along_y, y_ids, True), (along_x, x_ids, False)
        return (along_x, x_ids, False), (along_y, y_ids, True)

    kept = []
    for piece in range(3):
        copy = pltpu.make_async_copy(source(piece), place(piece, me_dp, me_fsdp), own_sem.at[piece])
        copy.start()
        kept.append(copy)
        first, second = dims(piece)
        push(piece, me_dp, me_fsdp, source(piece), z_ids + first[1] + second[1] + [partner])
    for other in along_z:
        for piece in range(3):
            first, second = dims(piece)
            row = other * 2 + core
            push(piece, me_dp, row, arrived(piece, me_dp, row), first[1] + second[1] + [partner])
    all_z = [z] + along_z
    for other in all_z:
        for piece in range(3):
            first, second = dims(piece)
            row = other * 2 + core
            for place_one in first[0]:
                column = place_one * low + x if first[2] else y * low + place_one
                push(piece, column, row, arrived(piece, column, row), second[1] + [partner])
    for other in all_z:
        for piece in range(3):
            first, second = dims(piece)
            own_first = y if first[2] else x
            row = other * 2 + core
            for place_two in second[0]:
                for place_one in [own_first] + first[0]:
                    column = (
                        place_one * low + place_two if first[2] else place_two * low + place_one
                    )
                    push(piece, column, row, arrived(piece, column, row), [partner])
    for other in all_z:
        for piece in range(3):
            for place_y in [y] + along_y:
                for place_x in [x] + along_x:
                    arrived(piece, place_y * low + place_x, other * 2 + 1 - core)
    for copy in kept:
        copy.wait()
    for copy in started:
        copy.wait_send()


def gather_all(shard, vec_shard, dp_size, fsdp_size):
    cut = shard.shape[0] // 2 // 16 * 16
    high, low = split_two(dp_size)
    depth = fsdp_size // 2
    sends = 0
    for first, second in ((low, high), (low, high), (high, low)):
        sends += (depth - 1) + depth * (first - 1) + depth * first * (second - 1)
        sends += depth * first * second
    return pl.pallas_call(
        partial(gather_kernel, dp_size, fsdp_size, cut),
        out_shape=(
            jax.ShapeDtypeStruct((fsdp_size, dp_size) + shard.shape, shard.dtype),
            jax.ShapeDtypeStruct((dp_size, fsdp_size) + vec_shard.shape, vec_shard.dtype),
        ),
        in_specs=[pl.BlockSpec(memory_space=pltpu.VMEM)] * 2,
        out_specs=(pl.BlockSpec(memory_space=pltpu.VMEM),) * 2,
        scratch_shapes=[
            pltpu.SemaphoreType.DMA((sends,)),
            pltpu.SemaphoreType.DMA((3, dp_size, fsdp_size)),
            pltpu.SemaphoreType.DMA((3,)),
        ],
        compiler_params=pltpu.CompilerParams(
            collective_id=0, has_side_effects=True, vmem_limit_bytes=40 << 20
        ),
        name="gather_all",
    )(shard, vec_shard)


def reduce_kernel(
    dp_size,
    fsdp_size,
    big_ref,
    small_ref,
    big_out_ref,
    small_out_ref,
    big_near,
    small_near,
    big_sum,
    small_sum,
    big_dp,
    small_dp,
    big_part,
    small_part,
    big_z,
    small_z,
    big_end,
    small_end,
    send_sem,
    near_sem,
    dp_sem,
    z_sem,
    big_sem,
    small_sem,
    own_sem,
):
    depth = fsdp_size // 2
    me_dp, me_fsdp = lax.axis_index("dp"), lax.axis_index("fsdp")
    z, core = me_fsdp // 2, lax.rem(me_fsdp, 2)
    along_dp = [lax.rem(me_dp + i, dp_size) for i in range(1, dp_size)]
    along_z = [lax.rem(z + i, depth) for i in range(1, depth)]
    partner = (me_dp, z * 2 + 1 - core)
    dp_ids = [(other, me_fsdp) for other in along_dp]
    z_ids = [(me_dp, other * 2 + core) for other in along_z]
    meet([partner] + dp_ids + z_ids)
    started = []

    def push(held, target, semaphore, peer):
        copy = pltpu.make_async_remote_copy(
            src_ref=held,
            dst_ref=target,
            send_sem=send_sem.at[len(started)],
            recv_sem=semaphore,
            device_id=peer,
            device_id_type=MESH,
        )
        copy.start()
        started.append(copy)

    def arrived(block, semaphore):
        pltpu.make_async_remote_copy(
            src_ref=block,
            dst_ref=block,
            send_sem=send_sem.at[0],
            recv_sem=semaphore,
            device_id=partner,
            device_id_type=MESH,
        ).wait_recv()

    def wide(block):
        return block.astype(jnp.float32)

    for other in along_dp + [me_dp]:
        push(big_ref.at[1 - core, other], big_near.at[other], near_sem.at[0, other], partner)
        push(small_ref.at[1 - core, other], small_near.at[other], near_sem.at[1, other], partner)
    for other, peer in zip(along_dp, dp_ids):
        arrived(big_near.at[other], near_sem.at[0, other])
        arrived(small_near.at[other], near_sem.at[1, other])
        for level in range(depth):
            big_sum[other, level] = (
                wide(big_ref[core, other, level]) + wide(big_near[other, level])
            ).astype(big_sum.dtype)
            small_sum[other, level] = (
                wide(small_ref[core, other, level]) + wide(small_near[other, level])
            ).astype(small_sum.dtype)
        for level in range(depth):
            push(
                big_sum.at[other, level],
                big_dp.at[me_dp, level],
                dp_sem.at[0, me_dp, level],
                peer,
            )
            push(
                small_sum.at[other, level],
                small_dp.at[me_dp, level],
                dp_sem.at[1, me_dp, level],
                peer,
            )
    arrived(big_near.at[me_dp], near_sem.at[0, me_dp])
    arrived(small_near.at[me_dp], near_sem.at[1, me_dp])

    def over_dp(level):
        big = wide(big_ref[core, me_dp, level]) + wide(big_near[me_dp, level])
        small = wide(small_ref[core, me_dp, level]) + wide(small_near[me_dp, level])
        for other in along_dp:
            arrived(big_dp.at[other, level], dp_sem.at[0, other, level])
            arrived(small_dp.at[other, level], dp_sem.at[1, other, level])
            big = big + wide(big_dp[other, level])
            small = small + wide(small_dp[other, level])
        return big, small

    for level, peer in zip(along_z, z_ids):
        big, small = over_dp(level)
        big_part[level] = big.astype(big_part.dtype)
        small_part[level] = small.astype(small_part.dtype)
        push(big_part.at[level], big_z.at[z], z_sem.at[0, z], peer)
        push(small_part.at[level], small_z.at[z], z_sem.at[1, z], peer)
    big, small = over_dp(z)
    for level in along_z:
        arrived(small_z.at[level], z_sem.at[1, level])
        small = small + wide(small_z[level])
    small_end[...] = small.astype(small_end.dtype)
    for peer in z_ids + dp_ids + [partner]:
        push(small_end, small_out_ref.at[core, me_dp, z], small_sem.at[core, me_dp, z], peer)
    for level in along_z:
        arrived(big_z.at[level], z_sem.at[0, level])
        big = big + wide(big_z[level])
    big_end[...] = big.astype(big_end.dtype)
    for peer in dp_ids:
        push(big_end, big_out_ref.at[me_dp], big_sem.at[me_dp], peer)
    kept = [
        pltpu.make_async_copy(small_end, small_out_ref.at[core, me_dp, z], own_sem.at[0]),
        pltpu.make_async_copy(big_end, big_out_ref.at[me_dp], own_sem.at[1]),
    ]
    for copy in kept:
        copy.start()
    for level in along_z:
        block = small_out_ref.at[core, me_dp, level]
        arrived(block, small_sem.at[core, me_dp, level])
        for peer in dp_ids + [partner]:
            push(block, block, small_sem.at[core, me_dp, level], peer)
    for level in [z] + along_z:
        for other in along_dp:
            block = small_out_ref.at[core, other, level]
            arrived(block, small_sem.at[core, other, level])
            push(block, block, small_sem.at[core, other, level], partner)
    for other in along_dp:
        arrived(big_out_ref.at[other], big_sem.at[other])
    for level in [z] + along_z:
        for other in [me_dp] + along_dp:
            arrived(
                small_out_ref.at[1 - core, other, level], small_sem.at[1 - core, other, level]
            )
    for copy in kept:
        copy.wait()
    for copy in started:
        copy.wait_send()


def reduce_all(big, small, dp_size, fsdp_size):
    depth = fsdp_size // 2
    sends = 2 * dp_size + 2 * (dp_size - 1) * depth + 2 * (depth - 1)
    sends += (depth - 1) + dp_size + (dp_size - 1)
    sends += (depth - 1) * dp_size + depth * (dp_size - 1)
    shapes = (big.shape[3:], small.shape[3:])
    low = big.dtype
    scratch = []
    for lead in ((dp_size, depth), (dp_size, depth), (dp_size, depth), (depth,), (depth,), ()):
        scratch += [pltpu.VMEM(lead + shape, low) for shape in shapes]
    return pl.pallas_call(
        partial(reduce_kernel, dp_size, fsdp_size),
        out_shape=(
            jax.ShapeDtypeStruct((dp_size,) + shapes[0], low),
            jax.ShapeDtypeStruct(small.shape, low),
        ),
        in_specs=[pl.BlockSpec(memory_space=pltpu.VMEM)] * 2,
        out_specs=(pl.BlockSpec(memory_space=pltpu.VMEM),) * 2,
        scratch_shapes=scratch
        + [
            pltpu.SemaphoreType.DMA((sends,)),
            pltpu.SemaphoreType.DMA((2, dp_size)),
            pltpu.SemaphoreType.DMA((2, dp_size, depth)),
            pltpu.SemaphoreType.DMA((2, depth)),
            pltpu.SemaphoreType.DMA((dp_size,)),
            pltpu.SemaphoreType.DMA((2, dp_size, depth)),
            pltpu.SemaphoreType.DMA((2,)),
        ],
        compiler_params=pltpu.CompilerParams(
            collective_id=1, has_side_effects=True, vmem_limit_bytes=40 << 20
        ),
        name="reduce_all",
    )(big, small)


def scalar_kernel(
    dp_size, fsdp_size, part_ref, out_ref, row_slots, row_sum, dp_slots, send_sem, row_sem, dp_sem
):
    me_dp, me_fsdp = lax.axis_index("dp"), lax.axis_index("fsdp")
    along_dp = [lax.rem(me_dp + i, dp_size) for i in range(1, dp_size)]
    along_fsdp = [lax.rem(me_fsdp + i, fsdp_size) for i in range(1, fsdp_size)]
    meet([(me_dp, other) for other in along_fsdp] + [(other, me_fsdp) for other in along_dp])
    started = []

    def exchange(held, slots, semaphores, me, others, peers):
        for peer in peers:
            copy = pltpu.make_async_remote_copy(
                src_ref=held,
                dst_ref=slots.at[me],
                send_sem=send_sem.at[len(started)],
                recv_sem=semaphores.at[me],
                device_id=peer,
                device_id_type=MESH,
            )
            copy.start()
            started.append(copy)
        slots[me] = held[...]
        for other in others:
            pltpu.make_async_remote_copy(
                src_ref=held,
                dst_ref=slots.at[other],
                send_sem=send_sem.at[0],
                recv_sem=semaphores.at[other],
                device_id=peers[0],
                device_id_type=MESH,
            ).wait_recv()
        total = slots[0]
        for place in range(1, len(others) + 1):
            total = total + slots[place]
        return total

    row_sum[...] = exchange(
        part_ref, row_slots, row_sem, me_fsdp, along_fsdp, [(me_dp, other) for other in along_fsdp]
    )
    out_ref[...] = exchange(
        row_sum, dp_slots, dp_sem, me_dp, along_dp, [(other, me_fsdp) for other in along_dp]
    )
    for copy in started:
        copy.wait_send()


def scalar_sums(values, dp_size, fsdp_size):
    lanes = jnp.arange(128, dtype=jnp.int32)[None, :]
    tile = sum(jnp.where(lanes == index, value, 0.0) for index, value in enumerate(values))
    tile = jnp.broadcast_to(tile, (8, 128))
    sums = pl.pallas_call(
        partial(scalar_kernel, dp_size, fsdp_size),
        out_shape=jax.ShapeDtypeStruct((8, 128), jnp.float32),
        in_specs=[pl.BlockSpec(memory_space=pltpu.VMEM)],
        out_specs=pl.BlockSpec(memory_space=pltpu.VMEM),
        scratch_shapes=[
            pltpu.VMEM((fsdp_size, 8, 128), jnp.float32),
            pltpu.VMEM((8, 128), jnp.float32),
            pltpu.VMEM((dp_size, 8, 128), jnp.float32),
            pltpu.SemaphoreType.DMA((fsdp_size + dp_size,)),
            pltpu.SemaphoreType.DMA((fsdp_size,)),
            pltpu.SemaphoreType.DMA((dp_size,)),
        ],
        compiler_params=pltpu.CompilerParams(collective_id=2, has_side_effects=True),
        name="scalar_sums",
    )(tile)
    return [sums[0, index] for index in range(len(values))]


def eigenbasis_update(
    gradient, master, moment, square, rotated_grads, col_start, first_correction, second_correction
):
    rotated = jnp.dot(gradient, rotated_grads, precision=highest_precision)
    moment_new = beta_one * moment + (1.0 - beta_one) * rotated
    square_new = beta_two * square + (1.0 - beta_two) * rotated * rotated
    step_ratio = (
        moment_new / first_correction / (jnp.sqrt(square_new / second_correction) + epsilon)
    )
    own_basis = lax.dynamic_slice_in_dim(rotated_grads, col_start, master.shape[1], 0)
    update = jnp.einsum("ri,ci->rc", step_ratio, own_basis, precision=highest_precision)
    master_new = master - rate_matrix * (update + decay_weight * master)
    return (master_new, master_new.astype(jnp.bfloat16), moment_new, square_new)


def adam_vectors(gradient, master, moment, square, first_correction, second_correction):
    decay_rows = jnp.where(
        jnp.arange(master.shape[0], dtype=jnp.int32)[:, None] < 2 * VOCAB, decay_weight, 0.0
    )
    moment_new = beta_one * moment + (1.0 - beta_one) * gradient
    square_new = beta_two * square + (1.0 - beta_two) * gradient * gradient
    step_ratio = (
        moment_new / first_correction / (jnp.sqrt(square_new / second_correction) + epsilon)
    )
    master_new = master - rate_vector * (step_ratio + decay_rows * master)
    return (master_new, master_new.astype(jnp.bfloat16), moment_new, square_new)


def local(
    input_tokens,
    item_numbers,
    loss_positions,
    target_tokens,
    input_projection,
    dilated_conv,
    output_projection,
    vectors,
    input_first_moment,
    input_second_moment,
    conv_first_moment,
    conv_second_moment,
    output_first_moment,
    output_second_moment,
    vector_first_moment,
    vector_second_moment,
    bases,
    eigenbasis_flags,
    optimizer_step,
):
    groups, col_index = lax.axis_size("dp"), lax.axis_index("dp")
    rows, row_index = lax.axis_size("fsdp"), lax.axis_index("fsdp")
    own_conv, own_in = dilated_conv.shape[0], input_projection.shape[0]
    shard = jnp.concatenate([dilated_conv, input_projection, output_projection], axis=0)
    all_weights, all_vectors = gather_all(
        shard.astype(jnp.bfloat16).T,
        vectors.astype(jnp.bfloat16).astype(jnp.float32).T,
        groups,
        rows,
    )

    def whole(begin, count):
        piece = lax.slice_in_dim(all_weights, begin, begin + count, axis=3)
        return piece.reshape(rows, -1, count).transpose(0, 2, 1).reshape(rows * count, -1)

    weight_conv = whole(0, own_conv)
    weight_in = whole(own_conv, own_in)
    weight_out = whole(own_conv + own_in, own_in)
    table_low = all_vectors.reshape(-1, all_vectors.shape[3]).T.astype(jnp.bfloat16)
    inner = weight_in.shape[1]
    width = weight_in.shape[0]
    start = 2 * VOCAB
    table = table_low.astype(jnp.float32)
    head = table_low[VOCAB:start]
    onehots = tap_onehots(input_tokens, item_numbers, loss_positions)
    onehots_low = onehots.astype(jnp.bfloat16)
    centre = CONV_TAPS // 2 * TABLE
    centre_low = onehots_low[:, centre : centre + TABLE]
    embedded = jnp.concatenate([table_low[:VOCAB], jnp.zeros((TABLE - VOCAB, width), jnp.bfloat16)], axis=0)
    first_act, first_back = jax.vjp(
        norm_gelu, embedded.astype(jnp.float32), table[start], table[start + 1]
    )
    first_low = first_act.astype(jnp.bfloat16)
    pre_inner = (
        jnp.dot(first_low, weight_in, preferred_element_type=jnp.float32)
        + table[start + 6, :inner]
    )
    second_act, second_back = jax.vjp(
        norm_gelu, pre_inner, table[start + 5, :inner], table[start + 5, inner:]
    )
    second_low = second_act.astype(jnp.bfloat16)
    picked_act = [
        jnp.dot(
            onehots_low[:, tap * TABLE : (tap + 1) * TABLE],
            second_low,
            preferred_element_type=jnp.float32,
        ).astype(jnp.bfloat16)
        for tap in range(CONV_TAPS)
    ]
    conv_input = (
        jnp.dot(
            jnp.concatenate(picked_act, axis=1), weight_conv, preferred_element_type=jnp.float32
        )
        + table[start + 6, inner:]
    )
    third_act, third_back = jax.vjp(
        norm_gelu, conv_input, table[start + 7, :inner], table[start + 7, inner:]
    )
    third_low = third_act.astype(jnp.bfloat16)
    branch = (
        jnp.einsum("ti,di->td", third_low, weight_out, preferred_element_type=jnp.float32)
        + table[start + 2]
    )
    picked_embedded = jnp.dot(centre_low, embedded, preferred_element_type=jnp.float32)
    final_out, final_back = jax.vjp(
        layer_norm, picked_embedded + branch, table[start + 3], table[start + 4]
    )
    picked = final_out.astype(jnp.bfloat16)
    logits = jnp.einsum("pd,vd->pv", picked, head, preferred_element_type=jnp.float32)
    valid = loss_positions.reshape(-1) >= 0
    summed_loss, loss_back = jax.vjp(
        partial(slot_loss, labels=target_tokens.reshape(-1), valid_slot=valid), logits
    )
    logit_grad = loss_back(jnp.ones((), jnp.float32))[0].astype(jnp.bfloat16)
    head_grad = jnp.einsum("pv,pd->vd", logit_grad, picked, preferred_element_type=jnp.float32)
    picked_grad = jnp.dot(logit_grad, head, preferred_element_type=jnp.float32)
    sum_grad, gain_four, bias_four = final_back(picked_grad)
    branch_low = sum_grad.astype(jnp.bfloat16)
    out_grad = jnp.einsum("td,ti->di", branch_low, third_low, preferred_element_type=jnp.float32)
    third_grad = jnp.dot(branch_low, weight_out, preferred_element_type=jnp.float32)
    conv_pre, gain_three, bias_three = third_back(third_grad)
    conv_low = conv_pre.astype(jnp.bfloat16)
    tap_grads = lax.dot_general(
        onehots_low, conv_low, (((0,), (0,)), ((), ())), preferred_element_type=jnp.float32
    )
    start_grads = jnp.einsum(
        "tv,td->vd", centre_low.astype(jnp.float32), sum_grad, precision=highest_precision
    )
    slot_count = jnp.sum(valid.astype(jnp.float32))
    wide_rows = jnp.concatenate(
        [
            start_grads[:VOCAB],
            head_grad,
            jnp.stack(
                [
                    column_sum(branch_low),
                    gain_four,
                    bias_four,
                    jnp.concatenate([gain_three, bias_three]),
                ]
            ),
        ],
        axis=0,
    )
    depth = rows // 2
    big = out_grad.astype(jnp.bfloat16).reshape(depth, 2, groups, -1, inner)
    flat = jnp.concatenate(
        [tap_grads[:, at : at + 128] for at in range(0, inner, 128)]
        + [wide_rows[:, at : at + 128] for at in range(0, width, 128)],
        axis=0,
    )
    piece = -(-flat.shape[0] // (groups * rows * 16)) * 16
    padding = jnp.zeros((piece * groups * rows - flat.shape[0], 128), jnp.float32)
    small = jnp.concatenate([flat, padding], axis=0).astype(jnp.bfloat16)
    out_rows, small = reduce_all(
        big.transpose(1, 2, 0, 3, 4), small.reshape(2, groups, depth, piece, 128), groups, rows
    )
    out_rows = out_rows.reshape(-1, inner).astype(jnp.float32)
    small = small.reshape(-1, 128).astype(jnp.float32)
    taps = tap_grads.shape[0]
    tap_grads = jnp.concatenate(
        [small[at * taps : (at + 1) * taps] for at in range(inner // 128)], axis=1
    )
    small = small[taps * (inner // 128) :]
    count = wide_rows.shape[0]
    wide_rows = jnp.concatenate(
        [small[at * count : (at + 1) * count] for at in range(width // 128)], axis=1
    )

    tap_view = tap_grads.reshape(CONV_TAPS, TABLE, inner)
    second_grad = sum(
        exact_dot(tap_view[tap], weight_conv[tap * inner : (tap + 1) * inner], (((1,), (1,)), ((), ())))
        for tap in range(CONV_TAPS)
    )
    inner_pre, gain_two, bias_two = second_back(second_grad)
    first_grad = exact_dot(inner_pre, weight_in, (((1,), (1,)), ((), ())))
    table_grad, gain_one, bias_one = first_back(first_grad)
    vec_sum = jnp.concatenate(
        [
            table_grad[:VOCAB] + wide_rows[:VOCAB],
            wide_rows[VOCAB:start],
            jnp.stack(
                [
                    gain_one,
                    bias_one,
                    wide_rows[start],
                    wide_rows[start + 1],
                    wide_rows[start + 2],
                    jnp.concatenate([gain_two, bias_two]),
                    jnp.concatenate(
                        [jnp.sum(inner_pre, axis=0), jnp.sum(tap_view[CONV_TAPS // 2], axis=0)]
                    ),
                    wide_rows[start + 3],
                ]
            ),
        ],
        axis=0,
    )
    own = width // (groups * rows)
    vec_own = lax.dynamic_slice_in_dim(vec_sum, (col_index * rows + row_index) * own, own, 1)

    row_low = lax.dynamic_slice_in_dim(first_low, row_index * (width // rows), width // rows, 1)
    in_rows = jnp.einsum(
        "vr,vi->ri", row_low.astype(jnp.float32), inner_pre, precision=highest_precision
    )
    placed = (
        jnp.eye(CONV_TAPS, dtype=jnp.bfloat16)[:, None, :, None] * second_low[None, :, None, :]
    ).reshape(CONV_TAPS * TABLE, CONV_TAPS * inner)
    conv_count = CONV_TAPS * inner // rows
    conv_low_rows = lax.dynamic_slice_in_dim(placed, row_index * conv_count, conv_count, 1)
    conv_rows = jnp.einsum(
        "vr,vi->ri", conv_low_rows.astype(jnp.float32), tap_grads, precision=highest_precision
    )

    col_width = input_projection.shape[1]
    col_start = col_index * col_width
    owned = [
        lax.dynamic_slice_in_dim(full_rows, col_start, col_width, 1)
        for full_rows in (in_rows, conv_rows, out_rows)
    ]
    square_local = sum((jnp.sum(piece * piece) for piece in owned)) + jnp.sum(vec_own * vec_own)
    square_total, summed_loss, slot_count = scalar_sums(
        (square_local, summed_loss, slot_count), groups, rows
    )
    grad_norm = jnp.sqrt(square_total) / slot_count
    factor = jnp.minimum(1.0, clip_limit / grad_norm) / slot_count
    step_value = optimizer_step[0].astype(jnp.float32)
    first_correction = 1.0 - beta_one**step_value
    second_correction = 1.0 - beta_two**step_value
    identity = jnp.eye(bases.shape[1], dtype=jnp.float32)
    rotated_grads = [
        jnp.where(eigenbasis_flags[mat_index] == 1, bases[mat_index], identity)
        for mat_index in range(3)
    ]
    master_in, copy_in, moment_in, square_in = eigenbasis_update(
        in_rows * factor,
        input_projection,
        input_first_moment,
        input_second_moment,
        rotated_grads[0],
        col_start,
        first_correction,
        second_correction,
    )
    updated_conv, conv_bfloat_copy, updated_conv_moment, updated_conv_square = eigenbasis_update(
        conv_rows * factor,
        dilated_conv,
        conv_first_moment,
        conv_second_moment,
        rotated_grads[1],
        col_start,
        first_correction,
        second_correction,
    )
    master_out, copy_out, moment_out, square_out = eigenbasis_update(
        out_rows * factor,
        output_projection,
        output_first_moment,
        output_second_moment,
        rotated_grads[2],
        col_start,
        first_correction,
        second_correction,
    )
    master_vec, copy_vec, moment_vec, square_vec = adam_vectors(
        vec_own * factor,
        vectors,
        vector_first_moment,
        vector_second_moment,
        first_correction,
        second_correction,
    )
    return (
        summed_loss / slot_count,
        grad_norm,
        master_in,
        copy_in,
        moment_in,
        square_in,
        updated_conv,
        conv_bfloat_copy,
        updated_conv_moment,
        updated_conv_square,
        master_out,
        copy_out,
        moment_out,
        square_out,
        master_vec,
        copy_vec,
        moment_vec,
        square_vec,
    )


def solution(mesh):
    placed = (
        P(None, ("dp", "fsdp")),
        P(None, ("dp", "fsdp")),
        P(None, ("dp", "fsdp")),
        P(None, ("dp", "fsdp")),
        P("fsdp", "dp"),
        P("fsdp", "dp"),
        P("fsdp", "dp"),
        P(None, ("dp", "fsdp")),
        P("fsdp", None),
        P("fsdp", None),
        P("fsdp", None),
        P("fsdp", None),
        P("fsdp", None),
        P("fsdp", None),
        P(None, ("dp", "fsdp")),
        P(None, ("dp", "fsdp")),
        P(),
        P(),
        P(),
    )
    return jax.shard_map(
        local,
        mesh=mesh,
        in_specs=placed,
        out_specs=(
            P(),
            P(),
            P("fsdp", "dp"),
            P("fsdp", "dp"),
            P("fsdp", None),
            P("fsdp", None),
            P("fsdp", "dp"),
            P("fsdp", "dp"),
            P("fsdp", None),
            P("fsdp", None),
            P("fsdp", "dp"),
            P("fsdp", "dp"),
            P("fsdp", None),
            P("fsdp", None),
            P(None, ("dp", "fsdp")),
            P(None, ("dp", "fsdp")),
            P(None, ("dp", "fsdp")),
            P(None, ("dp", "fsdp")),
        ),
        check_vma=False,
    )
```

```python
from functools import partial

import jax
import jax.numpy as jnp
from jax import lax
from jax.experimental import pallas as pl
from jax.experimental.pallas import tpu as pltpu
from jax.sharding import PartitionSpec as P

VOCAB = 30
CONV_TAPS = 5
DILATION = 8
TABLE = 32
MESH = pl.DeviceIdType.MESH


beta_one = 0.9
beta_two = 0.95
epsilon = 1e-08
rate_matrix = 0.02
rate_vector = 0.5
decay_weight = 0.01
clip_limit = 0.02
norm_eps = 1e-05
highest_precision = lax.Precision.HIGHEST


def layer_norm(values, norm_gain, norm_bias):
    centre = values - jnp.mean(values, axis=-1, keepdims=True)
    spread = jnp.mean(centre * centre, axis=-1, keepdims=True)
    return centre * lax.rsqrt(spread + norm_eps) * norm_gain + norm_bias


def norm_gelu(values, norm_gain, norm_bias):
    return jax.nn.gelu(layer_norm(values, norm_gain, norm_bias), approximate=True)


def moved_groups(values, step):
    if step > 0:
        return jnp.concatenate([values[:, step:], jnp.full_like(values[:, :step], -1)], axis=1)
    if step < 0:
        return jnp.concatenate([jnp.full_like(values[:, :-step], -1), values[:, :step]], axis=1)
    return values


def tap_onehots(tokens, items, positions):
    batches, slots = positions.shape
    stride = tokens.shape[1] // slots
    token_groups = tokens.reshape(batches, slots, stride)
    item_groups = items.reshape(batches, slots, stride)
    valid = positions >= 0
    residue = jnp.where(valid, positions - stride * jnp.arange(slots, dtype=jnp.int32)[None], -1)
    chosen = residue[:, :, None] == jnp.arange(stride, dtype=jnp.int32)[None, None]
    own_item = jnp.sum(jnp.where(chosen, item_groups, 0), axis=2)
    identities = jnp.arange(TABLE, dtype=jnp.int32)
    result = []
    for tap in range(CONV_TAPS):
        step = (tap - CONV_TAPS // 2) * DILATION // stride
        item = jnp.sum(jnp.where(chosen, moved_groups(item_groups, step), 0), axis=2)
        token = jnp.sum(jnp.where(chosen, moved_groups(token_groups, step), 0), axis=2)
        keep = valid & (item == own_item) & (own_item >= 0)
        result.append(jnp.where(keep, token, -1)[:, :, None] == identities)
    return jnp.concatenate(result, axis=2).reshape(batches * slots, CONV_TAPS * TABLE)


def exact_dot(left, right, contract):
    high = left.astype(jnp.bfloat16)
    low = (left - high.astype(jnp.float32)).astype(jnp.bfloat16)
    return lax.dot_general(high, right, contract, preferred_element_type=jnp.float32) + lax.dot_general(
        low, right, contract, preferred_element_type=jnp.float32
    )


def column_sum(values):
    return jnp.sum(values, axis=0, dtype=jnp.float32)


def split_two(count):
    high = int(count**0.5)
    while count % high:
        high -= 1
    return high, count // high


def spread_peers(dp_size, fsdp_size):
    high, low = split_two(dp_size)
    depth = fsdp_size // 2
    me_dp, me_fsdp = lax.axis_index("dp"), lax.axis_index("fsdp")
    z, core = me_fsdp // 2, lax.rem(me_fsdp, 2)
    y, x = me_dp // low, lax.rem(me_dp, low)
    along_z = [lax.rem(z + i, depth) for i in range(1, depth)]
    along_y = [lax.rem(y + i, high) for i in range(1, high)]
    along_x = [lax.rem(x + i, low) for i in range(1, low)]
    return (z, y, x, core, low, along_z, along_y, along_x)


def meet(peers):
    barrier = pltpu.get_barrier_semaphore()
    for peer in peers:
        pl.semaphore_signal(barrier, inc=1, device_id=peer, device_id_type=MESH)
    pl.semaphore_wait(barrier, len(peers))


def gather_kernel(
    dp_size, fsdp_size, cut, shard_ref, vec_ref, out_ref, vec_out_ref, send_sem, recv_sem, own_sem
):
    z, y, x, core, low, along_z, along_y, along_x = spread_peers(dp_size, fsdp_size)
    me_dp, me_fsdp = y * low + x, z * 2 + core
    z_ids = [(me_dp, other * 2 + core) for other in along_z]
    y_ids = [(other * low + x, me_fsdp) for other in along_y]
    x_ids = [(y * low + other, me_fsdp) for other in along_x]
    partner = (me_dp, z * 2 + 1 - core)
    meet(z_ids + y_ids + x_ids + [partner])
    parts = ((0, cut), (cut, shard_ref.shape[0] - cut))

    def place(piece, column, row):
        if piece == 0:
            return vec_out_ref.at[column, row]
        begin, size = parts[piece - 1]
        return out_ref.at[row, column, pl.ds(begin, size)]

    def source(piece):
        if piece == 0:
            return vec_ref
        begin, size = parts[piece - 1]
        return shard_ref.at[pl.ds(begin, size)]

    started = []

    def push(piece, column, row, held, peers):
        for peer in peers:
            copy = pltpu.make_async_remote_copy(
                src_ref=held,
                dst_ref=place(piece, column, row),
                send_sem=send_sem.at[len(started)],
                recv_sem=recv_sem.at[piece, column, row],
                device_id=peer,
                device_id_type=MESH,
            )
            copy.start()
            started.append(copy)

    def arrived(piece, column, row):
        block = place(piece, column, row)
        pltpu.make_async_remote_copy(
            src_ref=block,
            dst_ref=block,
            send_sem=send_sem.at[0],
            recv_sem=recv_sem.at[piece, column, row],
            device_id=partner,
            device_id_type=MESH,
        ).wait_recv()
        return block

    def dims(piece):
        if piece == 2:
            return (along_y, y_ids, True), (along_x, x_ids, False)
        return (along_x, x_ids, False), (along_y, y_ids, True)

    kept = []
    for piece in range(3):
        copy = pltpu.make_async_copy(source(piece), place(piece, me_dp, me_fsdp), own_sem.at[piece])
        copy.start()
        kept.append(copy)
        first, second = dims(piece)
        push(piece, me_dp, me_fsdp, source(piece), z_ids + first[1] + second[1] + [partner])
    for other in along_z:
        for piece in range(3):
            first, second = dims(piece)
            row = other * 2 + core
            push(piece, me_dp, row, arrived(piece, me_dp, row), first[1] + second[1] + [partner])
    all_z = [z] + along_z
    for other in all_z:
        for piece in range(3):
            first, second = dims(piece)
            row = other * 2 + core
            for place_one in first[0]:
                column = place_one * low + x if first[2] else y * low + place_one
                push(piece, column, row, arrived(piece, column, row), second[1] + [partner])
    for other in all_z:
        for piece in range(3):
            first, second = dims(piece)
            own_first = y if first[2] else x
            row = other * 2 + core
            for place_two in second[0]:
                for place_one in [own_first] + first[0]:
                    column = (
                        place_one * low + place_two if first[2] else place_two * low + place_one
                    )
                    push(piece, column, row, arrived(piece, column, row), [partner])
    for other in all_z:
        for piece in range(3):
            for place_y in [y] + along_y:
                for place_x in [x] + along_x:
                    arrived(piece, place_y * low + place_x, other * 2 + 1 - core)
    for copy in kept:
        copy.wait()
    for copy in started:
        copy.wait_send()


def gather_all(shard, vec_shard, dp_size, fsdp_size):
    cut = shard.shape[0] // 2 // 16 * 16
    high, low = split_two(dp_size)
    depth = fsdp_size // 2
    sends = 0
    for first, second in ((low, high), (low, high), (high, low)):
        sends += (depth - 1) + depth * (first - 1) + depth * first * (second - 1)
        sends += depth * first * second
    return pl.pallas_call(
        partial(gather_kernel, dp_size, fsdp_size, cut),
        out_shape=(
            jax.ShapeDtypeStruct((fsdp_size, dp_size) + shard.shape, shard.dtype),
            jax.ShapeDtypeStruct((dp_size, fsdp_size) + vec_shard.shape, vec_shard.dtype),
        ),
        in_specs=[pl.BlockSpec(memory_space=pltpu.VMEM)] * 2,
        out_specs=(pl.BlockSpec(memory_space=pltpu.VMEM),) * 2,
        scratch_shapes=[
            pltpu.SemaphoreType.DMA((sends,)),
            pltpu.SemaphoreType.DMA((3, dp_size, fsdp_size)),
            pltpu.SemaphoreType.DMA((3,)),
        ],
        compiler_params=pltpu.CompilerParams(
            collective_id=0, has_side_effects=True, vmem_limit_bytes=40 << 20
        ),
        name="gather_all",
    )(shard, vec_shard)


def reduce_kernel(
    dp_size,
    fsdp_size,
    big_ref,
    small_ref,
    big_out_ref,
    small_out_ref,
    big_near,
    small_near,
    big_sum,
    small_sum,
    big_dp,
    small_dp,
    big_part,
    small_part,
    big_z,
    small_z,
    big_end,
    small_end,
    send_sem,
    near_sem,
    dp_sem,
    z_sem,
    big_sem,
    small_sem,
    own_sem,
):
    depth = fsdp_size // 2
    me_dp, me_fsdp = lax.axis_index("dp"), lax.axis_index("fsdp")
    z, core = me_fsdp // 2, lax.rem(me_fsdp, 2)
    along_dp = [lax.rem(me_dp + i, dp_size) for i in range(1, dp_size)]
    along_z = [lax.rem(z + i, depth) for i in range(1, depth)]
    partner = (me_dp, z * 2 + 1 - core)
    dp_ids = [(other, me_fsdp) for other in along_dp]
    z_ids = [(me_dp, other * 2 + core) for other in along_z]
    meet([partner] + dp_ids + z_ids)
    started = []

    def push(held, target, semaphore, peer):
        copy = pltpu.make_async_remote_copy(
            src_ref=held,
            dst_ref=target,
            send_sem=send_sem.at[len(started)],
            recv_sem=semaphore,
            device_id=peer,
            device_id_type=MESH,
        )
        copy.start()
        started.append(copy)

    def arrived(block, semaphore):
        pltpu.make_async_remote_copy(
            src_ref=block,
            dst_ref=block,
            send_sem=send_sem.at[0],
            recv_sem=semaphore,
            device_id=partner,
            device_id_type=MESH,
        ).wait_recv()

    def wide(block):
        return block.astype(jnp.float32)

    for other in along_dp + [me_dp]:
        push(big_ref.at[1 - core, other], big_near.at[other], near_sem.at[0, other], partner)
        push(small_ref.at[1 - core, other], small_near.at[other], near_sem.at[1, other], partner)
    for other, peer in zip(along_dp, dp_ids):
        arrived(big_near.at[other], near_sem.at[0, other])
        arrived(small_near.at[other], near_sem.at[1, other])
        for level in range(depth):
            big_sum[other, level] = (
                wide(big_ref[core, other, level]) + wide(big_near[other, level])
            ).astype(big_sum.dtype)
            small_sum[other, level] = (
                wide(small_ref[core, other, level]) + wide(small_near[other, level])
            ).astype(small_sum.dtype)
        for level in range(depth):
            push(
                big_sum.at[other, level],
                big_dp.at[me_dp, level],
                dp_sem.at[0, me_dp, level],
                peer,
            )
            push(
                small_sum.at[other, level],
                small_dp.at[me_dp, level],
                dp_sem.at[1, me_dp, level],
                peer,
            )
    arrived(big_near.at[me_dp], near_sem.at[0, me_dp])
    arrived(small_near.at[me_dp], near_sem.at[1, me_dp])

    def over_dp(level):
        big = wide(big_ref[core, me_dp, level]) + wide(big_near[me_dp, level])
        small = wide(small_ref[core, me_dp, level]) + wide(small_near[me_dp, level])
        for other in along_dp:
            arrived(big_dp.at[other, level], dp_sem.at[0, other, level])
            arrived(small_dp.at[other, level], dp_sem.at[1, other, level])
            big = big + wide(big_dp[other, level])
            small = small + wide(small_dp[other, level])
        return big, small

    for level, peer in zip(along_z, z_ids):
        big, small = over_dp(level)
        big_part[level] = big.astype(big_part.dtype)
        small_part[level] = small.astype(small_part.dtype)
        push(big_part.at[level], big_z.at[z], z_sem.at[0, z], peer)
        push(small_part.at[level], small_z.at[z], z_sem.at[1, z], peer)
    big, small = over_dp(z)
    for level in along_z:
        arrived(small_z.at[level], z_sem.at[1, level])
        small = small + wide(small_z[level])
    small_end[...] = small.astype(small_end.dtype)
    for peer in z_ids + dp_ids + [partner]:
        push(small_end, small_out_ref.at[core, me_dp, z], small_sem.at[core, me_dp, z], peer)
    for level in along_z:
        arrived(big_z.at[level], z_sem.at[0, level])
        big = big + wide(big_z[level])
    big_end[...] = big.astype(big_end.dtype)
    for peer in dp_ids:
        push(big_end, big_out_ref.at[me_dp], big_sem.at[me_dp], peer)
    kept = [
        pltpu.make_async_copy(small_end, small_out_ref.at[core, me_dp, z], own_sem.at[0]),
        pltpu.make_async_copy(big_end, big_out_ref.at[me_dp], own_sem.at[1]),
    ]
    for copy in kept:
        copy.start()
    for level in along_z:
        block = small_out_ref.at[core, me_dp, level]
        arrived(block, small_sem.at[core, me_dp, level])
        for peer in dp_ids + [partner]:
            push(block, block, small_sem.at[core, me_dp, level], peer)
    for level in [z] + along_z:
        for other in along_dp:
            block = small_out_ref.at[core, other, level]
            arrived(block, small_sem.at[core, other, level])
            push(block, block, small_sem.at[core, other, level], partner)
    for other in along_dp:
        arrived(big_out_ref.at[other], big_sem.at[other])
    for level in [z] + along_z:
        for other in [me_dp] + along_dp:
            arrived(
                small_out_ref.at[1 - core, other, level], small_sem.at[1 - core, other, level]
            )
    for copy in kept:
        copy.wait()
    for copy in started:
        copy.wait_send()


def reduce_all(big, small, dp_size, fsdp_size):
    depth = fsdp_size // 2
    sends = 2 * dp_size + 2 * (dp_size - 1) * depth + 2 * (depth - 1)
    sends += (depth - 1) + dp_size + (dp_size - 1)
    sends += (depth - 1) * dp_size + depth * (dp_size - 1)
    shapes = (big.shape[3:], small.shape[3:])
    low = big.dtype
    scratch = []
    for lead in ((dp_size, depth), (dp_size, depth), (dp_size, depth), (depth,), (depth,), ()):
        scratch += [pltpu.VMEM(lead + shape, low) for shape in shapes]
    return pl.pallas_call(
        partial(reduce_kernel, dp_size, fsdp_size),
        out_shape=(
            jax.ShapeDtypeStruct((dp_size,) + shapes[0], low),
            jax.ShapeDtypeStruct(small.shape, low),
        ),
        in_specs=[pl.BlockSpec(memory_space=pltpu.VMEM)] * 2,
        out_specs=(pl.BlockSpec(memory_space=pltpu.VMEM),) * 2,
        scratch_shapes=scratch
        + [
            pltpu.SemaphoreType.DMA((sends,)),
            pltpu.SemaphoreType.DMA((2, dp_size)),
            pltpu.SemaphoreType.DMA((2, dp_size, depth)),
            pltpu.SemaphoreType.DMA((2, depth)),
            pltpu.SemaphoreType.DMA((dp_size,)),
            pltpu.SemaphoreType.DMA((2, dp_size, depth)),
            pltpu.SemaphoreType.DMA((2,)),
        ],
        compiler_params=pltpu.CompilerParams(
            collective_id=1, has_side_effects=True, vmem_limit_bytes=40 << 20
        ),
        name="reduce_all",
    )(big, small)


def scalar_kernel(
    dp_size, fsdp_size, part_ref, out_ref, row_slots, row_sum, dp_slots, send_sem, row_sem, dp_sem
):
    me_dp, me_fsdp = lax.axis_index("dp"), lax.axis_index("fsdp")
    along_dp = [lax.rem(me_dp + i, dp_size) for i in range(1, dp_size)]
    along_fsdp = [lax.rem(me_fsdp + i, fsdp_size) for i in range(1, fsdp_size)]
    meet([(me_dp, other) for other in along_fsdp] + [(other, me_fsdp) for other in along_dp])
    started = []

    def exchange(held, slots, semaphores, me, others, peers):
        for peer in peers:
            copy = pltpu.make_async_remote_copy(
                src_ref=held,
                dst_ref=slots.at[me],
                send_sem=send_sem.at[len(started)],
                recv_sem=semaphores.at[me],
                device_id=peer,
                device_id_type=MESH,
            )
            copy.start()
            started.append(copy)
        slots[me] = held[...]
        for other in others:
            pltpu.make_async_remote_copy(
                src_ref=held,
                dst_ref=slots.at[other],
                send_sem=send_sem.at[0],
                recv_sem=semaphores.at[other],
                device_id=peers[0],
                device_id_type=MESH,
            ).wait_recv()
        total = slots[0]
        for place in range(1, len(others) + 1):
            total = total + slots[place]
        return total

    row_sum[...] = exchange(
        part_ref, row_slots, row_sem, me_fsdp, along_fsdp, [(me_dp, other) for other in along_fsdp]
    )
    out_ref[...] = exchange(
        row_sum, dp_slots, dp_sem, me_dp, along_dp, [(other, me_fsdp) for other in along_dp]
    )
    for copy in started:
        copy.wait_send()


def scalar_sums(values, dp_size, fsdp_size):
    lanes = jnp.arange(128, dtype=jnp.int32)[None, :]
    tile = sum(jnp.where(lanes == index, value, 0.0) for index, value in enumerate(values))
    tile = jnp.broadcast_to(tile, (8, 128))
    sums = pl.pallas_call(
        partial(scalar_kernel, dp_size, fsdp_size),
        out_shape=jax.ShapeDtypeStruct((8, 128), jnp.float32),
        in_specs=[pl.BlockSpec(memory_space=pltpu.VMEM)],
        out_specs=pl.BlockSpec(memory_space=pltpu.VMEM),
        scratch_shapes=[
            pltpu.VMEM((fsdp_size, 8, 128), jnp.float32),
            pltpu.VMEM((8, 128), jnp.float32),
            pltpu.VMEM((dp_size, 8, 128), jnp.float32),
            pltpu.SemaphoreType.DMA((fsdp_size + dp_size,)),
            pltpu.SemaphoreType.DMA((fsdp_size,)),
            pltpu.SemaphoreType.DMA((dp_size,)),
        ],
        compiler_params=pltpu.CompilerParams(collective_id=2, has_side_effects=True),
        name="scalar_sums",
    )(tile)
    return [sums[0, index] for index in range(len(values))]


def three_parts(values):
    high = values.astype(jnp.bfloat16)
    rest = values - high.astype(jnp.float32)
    middle = rest.astype(jnp.bfloat16)
    return high, middle, (rest - middle.astype(jnp.float32)).astype(jnp.bfloat16)


def product(left, right, left_axis, right_axis):
    return lax.dot_general(
        left,
        right,
        (((left_axis,), (right_axis,)), ((), ())),
        preferred_element_type=jnp.float32,
    )


def local_step_kernel(
    chunk,
    embed_ref,
    head_ref,
    rows_ref,
    onehot_ref,
    target_ref,
    weight_ref,
    big_ref,
    taps_ref,
    wide_ref,
    loss_ref,
    inner_ref,
    first_ref,
    placed_ref,
    spread,
    tap_table,
    kept_third,
    kept_grad,
    sums,
):
    fsdp_size, inner, packed = weight_ref.shape
    width = embed_ref.shape[1]
    own = width // fsdp_size
    own_conv = packed - 2 * own
    slots = onehot_ref.shape[0]
    gain_one, bias_one = rows_ref[0:1, :], rows_ref[1:2, :]
    first_low = norm_gelu(embed_ref[...], gain_one, bias_one).astype(jnp.bfloat16)
    pre_inner = jnp.broadcast_to(rows_ref[6:7, :inner], (TABLE, inner))
    for row in range(fsdp_size):
        block = first_low[:, row * own : (row + 1) * own]
        first_ref[row] = block
        pre_inner = pre_inner + product(
            block, weight_ref[row, :, own_conv : own_conv + own], 1, 1
        )
    inner_ref[...] = pre_inner
    second_low = norm_gelu(pre_inner, rows_ref[5:6, :inner], rows_ref[5:6, inner:]).astype(
        jnp.bfloat16
    )
    spread[...] = jnp.zeros_like(spread)
    for tap in range(CONV_TAPS):
        spread[tap * TABLE : (tap + 1) * TABLE, tap * inner : (tap + 1) * inner] = second_low
    total = jnp.zeros((CONV_TAPS * TABLE, inner), jnp.float32)
    for row in range(fsdp_size):
        block = spread[:, row * own_conv : (row + 1) * own_conv]
        placed_ref[row] = block
        total = total + product(block, weight_ref[row, :, :own_conv], 1, 1)
    tap_table[...] = jnp.concatenate(three_parts(total), axis=1)
    sums[...] = jnp.zeros_like(sums)
    taps_ref[...] = jnp.zeros_like(taps_ref)
    wide_ref[...] = jnp.zeros_like(wide_ref)
    embed_low = embed_ref[...].astype(jnp.bfloat16)
    head = head_ref[...]
    gain_four, bias_four = rows_ref[3:4, :], rows_ref[4:5, :]

    def one_chunk(index, carry):
        here = pl.ds(pl.multiple_of(index * chunk, chunk), chunk)
        onehot = onehot_ref[here, :]
        centre = onehot[:, CONV_TAPS // 2 * TABLE : (CONV_TAPS // 2 + 1) * TABLE]
        parts = product(onehot, tap_table[...], 1, 0)
        conv_input = (
            parts[:, :inner]
            + parts[:, inner : 2 * inner]
            + parts[:, 2 * inner :]
            + rows_ref[6:7, inner:]
        )
        third_act, third_back = jax.vjp(
            norm_gelu, conv_input, rows_ref[7:8, :inner], rows_ref[7:8, inner:]
        )
        third_low = third_act.astype(jnp.bfloat16)
        kept_third[here, :] = third_low
        branch = jnp.concatenate(
            [
                product(third_low, weight_ref[row, :, own_conv + own :], 1, 0)
                for row in range(fsdp_size)
            ],
            axis=1,
        )
        summed = product(centre, embed_low, 1, 0) + branch + rows_ref[2:3, :]
        final, final_back = jax.vjp(layer_norm, summed, gain_four, bias_four)
        picked = final.astype(jnp.bfloat16)
        logits = product(picked, head, 1, 1)
        lanes = lax.broadcasted_iota(jnp.int32, logits.shape, 1)
        logits = jnp.where(lanes < VOCAB, logits, -1e30)
        target = target_ref[here, :]
        valid = target >= 0
        highest = jnp.max(logits, axis=1, keepdims=True)
        powers = jnp.exp(logits - highest)
        power_sum = jnp.sum(powers, axis=1, keepdims=True)
        hits = lanes == target
        chosen = jnp.sum(jnp.where(hits, logits, 0.0), axis=1, keepdims=True)
        losses = jnp.where(valid, jnp.log(power_sum) + highest - chosen, 0.0)
        logit_grad = jnp.where(valid, powers / power_sum - hits.astype(jnp.float32), 0.0).astype(
            jnp.bfloat16
        )
        picked_grad = product(logit_grad, head, 1, 0)
        sum_grad, gain_grad, bias_grad = final_back(picked_grad)
        branch_low = sum_grad.astype(jnp.bfloat16)
        kept_grad[here, :] = branch_low
        third_grad = jnp.zeros((chunk, inner), jnp.float32)
        for row in range(fsdp_size):
            third_grad = third_grad + product(
                branch_low[:, row * own : (row + 1) * own],
                weight_ref[row, :, own_conv + own :],
                1,
                1,
            )
        conv_pre, gain_three, bias_three = third_back(third_grad)
        taps_ref[...] += product(onehot, conv_pre.astype(jnp.bfloat16), 0, 0)
        high, middle, low = three_parts(sum_grad)
        wide_ref[0:TABLE, :] += (
            product(centre, high, 0, 0) + product(centre, middle, 0, 0) + product(centre, low, 0, 0)
        )
        wide_ref[TABLE : 2 * TABLE, :] += product(logit_grad, picked, 0, 0)
        wide_ref[2 * TABLE : 2 * TABLE + 1, :] += jnp.sum(
            branch_low.astype(jnp.float32), axis=0, keepdims=True
        )
        wide_ref[2 * TABLE + 1 : 2 * TABLE + 2, :] += gain_grad
        wide_ref[2 * TABLE + 2 : 2 * TABLE + 3, :] += bias_grad
        wide_ref[2 * TABLE + 3 : 2 * TABLE + 4, :inner] += gain_three
        wide_ref[2 * TABLE + 3 : 2 * TABLE + 4, inner:] += bias_three
        sums[0:1, :] += jnp.sum(jnp.broadcast_to(losses, (chunk, 128)), axis=0, keepdims=True)
        sums[1:2, :] += jnp.sum(
            jnp.broadcast_to(valid.astype(jnp.float32), (chunk, 128)), axis=0, keepdims=True
        )
        return carry

    lax.fori_loop(0, slots // chunk, one_chunk, 0)
    loss_ref[...] = sums[...]
    third_all = kept_third[...]

    for row in range(fsdp_size):
        big_ref[row] = product(
            kept_grad[:, row * own : (row + 1) * own], third_all, 0, 0
        ).astype(jnp.bfloat16)


def local_step(embed, head, rows, onehots, targets, weights):
    fsdp_size, inner, packed = weights.shape
    slots, width = onehots.shape[0], embed.shape[1]
    own = width // fsdp_size
    own_conv = packed - 2 * own
    shape = jax.ShapeDtypeStruct
    vmem = pl.BlockSpec(memory_space=pltpu.VMEM)
    return pl.pallas_call(
        partial(local_step_kernel, min(slots, 128)),
        out_shape=(
            shape((fsdp_size, own, inner), jnp.bfloat16),
            shape((CONV_TAPS * TABLE, inner), jnp.float32),
            shape((2 * TABLE + 8, width), jnp.float32),
            shape((8, 128), jnp.float32),
            shape((TABLE, inner), jnp.float32),
            shape((fsdp_size, TABLE, own), jnp.bfloat16),
            shape((fsdp_size, CONV_TAPS * TABLE, own_conv), jnp.bfloat16),
        ),
        in_specs=[vmem] * 6,
        out_specs=(vmem,) * 7,
        scratch_shapes=[
            pltpu.VMEM((CONV_TAPS * TABLE, CONV_TAPS * inner), jnp.bfloat16),
            pltpu.VMEM((CONV_TAPS * TABLE, 3 * inner), jnp.bfloat16),
            pltpu.VMEM((slots, inner), jnp.bfloat16),
            pltpu.VMEM((slots, width), jnp.bfloat16),
            pltpu.VMEM((8, 128), jnp.float32),
        ],
        compiler_params=pltpu.CompilerParams(vmem_limit_bytes=48 << 20),
        name="local_step",
    )(embed, head, rows, onehots, targets, weights)


def eigenbasis_update(
    gradient, master, moment, square, rotated_grads, col_start, first_correction, second_correction
):
    rotated = jnp.dot(gradient, rotated_grads, precision=highest_precision)
    moment_new = beta_one * moment + (1.0 - beta_one) * rotated
    square_new = beta_two * square + (1.0 - beta_two) * rotated * rotated
    step_ratio = (
        moment_new / first_correction / (jnp.sqrt(square_new / second_correction) + epsilon)
    )
    own_basis = lax.dynamic_slice_in_dim(rotated_grads, col_start, master.shape[1], 0)
    update = jnp.einsum("ri,ci->rc", step_ratio, own_basis, precision=highest_precision)
    master_new = master - rate_matrix * (update + decay_weight * master)
    return (master_new, master_new.astype(jnp.bfloat16), moment_new, square_new)


def adam_vectors(gradient, master, moment, square, first_correction, second_correction):
    decay_rows = jnp.where(
        jnp.arange(master.shape[0], dtype=jnp.int32)[:, None] < 2 * VOCAB, decay_weight, 0.0
    )
    moment_new = beta_one * moment + (1.0 - beta_one) * gradient
    square_new = beta_two * square + (1.0 - beta_two) * gradient * gradient
    step_ratio = (
        moment_new / first_correction / (jnp.sqrt(square_new / second_correction) + epsilon)
    )
    master_new = master - rate_vector * (step_ratio + decay_rows * master)
    return (master_new, master_new.astype(jnp.bfloat16), moment_new, square_new)


def local(
    input_tokens,
    item_numbers,
    loss_positions,
    target_tokens,
    input_projection,
    dilated_conv,
    output_projection,
    vectors,
    input_first_moment,
    input_second_moment,
    conv_first_moment,
    conv_second_moment,
    output_first_moment,
    output_second_moment,
    vector_first_moment,
    vector_second_moment,
    bases,
    eigenbasis_flags,
    optimizer_step,
):
    groups, col_index = lax.axis_size("dp"), lax.axis_index("dp")
    rows, row_index = lax.axis_size("fsdp"), lax.axis_index("fsdp")
    own_conv, own_in = dilated_conv.shape[0], input_projection.shape[0]
    shard = jnp.concatenate([dilated_conv, input_projection, output_projection], axis=0)
    all_weights, all_vectors = gather_all(
        shard.astype(jnp.bfloat16).T,
        vectors.astype(jnp.bfloat16).astype(jnp.float32).T,
        groups,
        rows,
    )

    width = own_in * rows
    inner = groups * input_projection.shape[1]
    start = 2 * VOCAB
    weights = all_weights.reshape(rows, inner, -1)
    table = all_vectors.reshape(width, -1).T
    spare = jnp.zeros((TABLE - VOCAB, width), jnp.float32)
    embedded = jnp.concatenate([table[:VOCAB], spare], axis=0)
    head = jnp.concatenate([table[VOCAB:start], spare], axis=0).astype(jnp.bfloat16)
    norm_rows = table[start:]
    onehots = tap_onehots(input_tokens, item_numbers, loss_positions)
    targets = jnp.where(loss_positions >= 0, target_tokens, -1).reshape(-1, 1)
    out_grad, tap_grads, wide_rows, loss_tile, pre_inner, first_low, placed = local_step(
        embedded, head, norm_rows, onehots.astype(jnp.bfloat16), targets, weights
    )
    summed_loss, slot_count = loss_tile[0, 0], loss_tile[1, 0]
    depth = rows // 2
    big = out_grad.reshape(depth, 2, groups, -1, inner)
    flat = jnp.concatenate(
        [tap_grads[:, at : at + 128] for at in range(0, inner, 128)]
        + [wide_rows[:, at : at + 128] for at in range(0, width, 128)],
        axis=0,
    )
    piece = -(-flat.shape[0] // (groups * rows * 16)) * 16
    padding = jnp.zeros((piece * groups * rows - flat.shape[0], 128), jnp.float32)
    small = jnp.concatenate([flat, padding], axis=0).astype(jnp.bfloat16)
    out_rows, small = reduce_all(
        big.transpose(1, 2, 0, 3, 4), small.reshape(2, groups, depth, piece, 128), groups, rows
    )
    out_rows = out_rows.reshape(-1, inner).astype(jnp.float32)
    small = small.reshape(-1, 128).astype(jnp.float32)
    taps = tap_grads.shape[0]
    tap_grads = jnp.concatenate(
        [small[at * taps : (at + 1) * taps] for at in range(inner // 128)], axis=1
    )
    small = small[taps * (inner // 128) :]
    count = wide_rows.shape[0]
    wide_rows = jnp.concatenate(
        [small[at * count : (at + 1) * count] for at in range(width // 128)], axis=1
    )

    weight_conv = weights[:, :, :own_conv].transpose(0, 2, 1).reshape(-1, inner)
    weight_in = weights[:, :, own_conv : own_conv + own_in].transpose(0, 2, 1).reshape(-1, inner)
    second_back = jax.vjp(norm_gelu, pre_inner, norm_rows[5, :inner], norm_rows[5, inner:])[1]
    first_back = jax.vjp(norm_gelu, embedded, norm_rows[0], norm_rows[1])[1]
    tap_view = tap_grads.reshape(CONV_TAPS, TABLE, inner)
    second_grad = sum(
        exact_dot(tap_view[tap], weight_conv[tap * inner : (tap + 1) * inner], (((1,), (1,)), ((), ())))
        for tap in range(CONV_TAPS)
    )
    inner_pre, gain_two, bias_two = second_back(second_grad)
    first_grad = exact_dot(inner_pre, weight_in, (((1,), (1,)), ((), ())))
    table_grad, gain_one, bias_one = first_back(first_grad)
    vec_sum = jnp.concatenate(
        [
            table_grad[:VOCAB] + wide_rows[:VOCAB],
            wide_rows[TABLE : TABLE + VOCAB],
            jnp.stack(
                [
                    gain_one,
                    bias_one,
                    wide_rows[2 * TABLE],
                    wide_rows[2 * TABLE + 1],
                    wide_rows[2 * TABLE + 2],
                    jnp.concatenate([gain_two, bias_two]),
                    jnp.concatenate(
                        [jnp.sum(inner_pre, axis=0), jnp.sum(tap_view[CONV_TAPS // 2], axis=0)]
                    ),
                    wide_rows[2 * TABLE + 3],
                ]
            ),
        ],
        axis=0,
    )
    own = width // (groups * rows)
    vec_own = lax.dynamic_slice_in_dim(vec_sum, (col_index * rows + row_index) * own, own, 1)

    row_low = lax.dynamic_index_in_dim(first_low, row_index, 0, False)
    in_rows = jnp.einsum(
        "vr,vi->ri", row_low.astype(jnp.float32), inner_pre, precision=highest_precision
    )
    placed_own = lax.dynamic_index_in_dim(placed, row_index, 0, False)
    conv_rows = jnp.einsum(
        "vr,vi->ri", placed_own.astype(jnp.float32), tap_grads, precision=highest_precision
    )

    col_width = input_projection.shape[1]
    col_start = col_index * col_width
    owned = [
        lax.dynamic_slice_in_dim(full_rows, col_start, col_width, 1)
        for full_rows in (in_rows, conv_rows, out_rows)
    ]
    square_local = sum((jnp.sum(piece * piece) for piece in owned)) + jnp.sum(vec_own * vec_own)
    square_total, summed_loss, slot_count = scalar_sums(
        (square_local, summed_loss, slot_count), groups, rows
    )
    grad_norm = jnp.sqrt(square_total) / slot_count
    factor = jnp.minimum(1.0, clip_limit / grad_norm) / slot_count
    step_value = optimizer_step[0].astype(jnp.float32)
    first_correction = 1.0 - beta_one**step_value
    second_correction = 1.0 - beta_two**step_value
    identity = jnp.eye(bases.shape[1], dtype=jnp.float32)
    rotated_grads = [
        jnp.where(eigenbasis_flags[mat_index] == 1, bases[mat_index], identity)
        for mat_index in range(3)
    ]
    master_in, copy_in, moment_in, square_in = eigenbasis_update(
        in_rows * factor,
        input_projection,
        input_first_moment,
        input_second_moment,
        rotated_grads[0],
        col_start,
        first_correction,
        second_correction,
    )
    updated_conv, conv_bfloat_copy, updated_conv_moment, updated_conv_square = eigenbasis_update(
        conv_rows * factor,
        dilated_conv,
        conv_first_moment,
        conv_second_moment,
        rotated_grads[1],
        col_start,
        first_correction,
        second_correction,
    )
    master_out, copy_out, moment_out, square_out = eigenbasis_update(
        out_rows * factor,
        output_projection,
        output_first_moment,
        output_second_moment,
        rotated_grads[2],
        col_start,
        first_correction,
        second_correction,
    )
    master_vec, copy_vec, moment_vec, square_vec = adam_vectors(
        vec_own * factor,
        vectors,
        vector_first_moment,
        vector_second_moment,
        first_correction,
        second_correction,
    )
    return (
        summed_loss / slot_count,
        grad_norm,
        master_in,
        copy_in,
        moment_in,
        square_in,
        updated_conv,
        conv_bfloat_copy,
        updated_conv_moment,
        updated_conv_square,
        master_out,
        copy_out,
        moment_out,
        square_out,
        master_vec,
        copy_vec,
        moment_vec,
        square_vec,
    )


def solution(mesh):
    placed = (
        P(None, ("dp", "fsdp")),
        P(None, ("dp", "fsdp")),
        P(None, ("dp", "fsdp")),
        P(None, ("dp", "fsdp")),
        P("fsdp", "dp"),
        P("fsdp", "dp"),
        P("fsdp", "dp"),
        P(None, ("dp", "fsdp")),
        P("fsdp", None),
        P("fsdp", None),
        P("fsdp", None),
        P("fsdp", None),
        P("fsdp", None),
        P("fsdp", None),
        P(None, ("dp", "fsdp")),
        P(None, ("dp", "fsdp")),
        P(),
        P(),
        P(),
    )
    return jax.shard_map(
        local,
        mesh=mesh,
        in_specs=placed,
        out_specs=(
            P(),
            P(),
            P("fsdp", "dp"),
            P("fsdp", "dp"),
            P("fsdp", None),
            P("fsdp", None),
            P("fsdp", "dp"),
            P("fsdp", "dp"),
            P("fsdp", None),
            P("fsdp", None),
            P("fsdp", "dp"),
            P("fsdp", "dp"),
            P("fsdp", None),
            P("fsdp", None),
            P(None, ("dp", "fsdp")),
            P(None, ("dp", "fsdp")),
            P(None, ("dp", "fsdp")),
            P(None, ("dp", "fsdp")),
        ),
        check_vma=False,
    )
```

```python
import math
from functools import partial

import jax
import jax.numpy as jnp
from jax import lax
from jax.experimental import pallas as pl
from jax.experimental.pallas import tpu as pltpu
from jax.sharding import PartitionSpec as P

VOCAB = 30
CONV_TAPS = 5
DILATION = 8
TABLE = 32
MESH = pl.DeviceIdType.MESH


beta_one = 0.9
beta_two = 0.95
epsilon = 1e-08
rate_matrix = 0.02
rate_vector = 0.5
decay_weight = 0.01
clip_limit = 0.02
norm_eps = 1e-05
highest_precision = lax.Precision.HIGHEST


def layer_norm(values, norm_gain, norm_bias):
    centre = values - jnp.mean(values, axis=-1, keepdims=True)
    spread = jnp.mean(centre * centre, axis=-1, keepdims=True)
    return centre * lax.rsqrt(spread + norm_eps) * norm_gain + norm_bias


def norm_gelu(values, norm_gain, norm_bias):
    return jax.nn.gelu(layer_norm(values, norm_gain, norm_bias), approximate=True)


def moved_groups(values, step):
    if step > 0:
        return jnp.concatenate([values[:, step:], jnp.full_like(values[:, :step], -1)], axis=1)
    if step < 0:
        return jnp.concatenate([jnp.full_like(values[:, :-step], -1), values[:, :step]], axis=1)
    return values


def tap_onehots(tokens, items, positions):
    batches, slots = positions.shape
    stride = tokens.shape[1] // slots
    token_groups = tokens.reshape(batches, slots, stride)
    item_groups = items.reshape(batches, slots, stride)
    valid = positions >= 0
    residue = jnp.where(valid, positions - stride * jnp.arange(slots, dtype=jnp.int32)[None], -1)
    chosen = residue[:, :, None] == jnp.arange(stride, dtype=jnp.int32)[None, None]
    own_item = jnp.sum(jnp.where(chosen, item_groups, 0), axis=2)
    identities = jnp.arange(TABLE, dtype=jnp.int32)
    result = []
    for tap in range(CONV_TAPS):
        step = (tap - CONV_TAPS // 2) * DILATION // stride
        item = jnp.sum(jnp.where(chosen, moved_groups(item_groups, step), 0), axis=2)
        token = jnp.sum(jnp.where(chosen, moved_groups(token_groups, step), 0), axis=2)
        keep = valid & (item == own_item) & (own_item >= 0)
        result.append(jnp.where(keep, token, -1)[:, :, None] == identities)
    return jnp.concatenate(result, axis=2).reshape(batches * slots, CONV_TAPS * TABLE)


def split_two(count):
    high = int(count**0.5)
    while count % high:
        high -= 1
    return high, count // high


def spread_peers(dp_size, fsdp_size):
    high, low = split_two(dp_size)
    depth = fsdp_size // 2
    me_dp, me_fsdp = lax.axis_index("dp"), lax.axis_index("fsdp")
    z, core = me_fsdp // 2, lax.rem(me_fsdp, 2)
    y, x = me_dp // low, lax.rem(me_dp, low)
    along_z = [lax.rem(z + i, depth) for i in range(1, depth)]
    along_y = [lax.rem(y + i, high) for i in range(1, high)]
    along_x = [lax.rem(x + i, low) for i in range(1, low)]
    return (z, y, x, core, low, along_z, along_y, along_x)


def meet(peers):
    barrier = pltpu.get_barrier_semaphore()
    for peer in peers:
        pl.semaphore_signal(barrier, inc=1, device_id=peer, device_id_type=MESH)
    pl.semaphore_wait(barrier, len(peers))


def gather_kernel(
    dp_size, fsdp_size, cut, shard_ref, vec_ref, out_ref, vec_out_ref, send_sem, recv_sem, own_sem
):
    z, y, x, core, low, along_z, along_y, along_x = spread_peers(dp_size, fsdp_size)
    me_dp, me_fsdp = y * low + x, z * 2 + core
    z_ids = [(me_dp, other * 2 + core) for other in along_z]
    y_ids = [(other * low + x, me_fsdp) for other in along_y]
    x_ids = [(y * low + other, me_fsdp) for other in along_x]
    partner = (me_dp, z * 2 + 1 - core)
    meet(z_ids + y_ids + x_ids + [partner])
    parts = ((0, cut), (cut, shard_ref.shape[0] - cut))

    def place(piece, column, row):
        if piece == 0:
            return vec_out_ref.at[column, row]
        begin, size = parts[piece - 1]
        return out_ref.at[row, column, pl.ds(begin, size)]

    def source(piece):
        if piece == 0:
            return vec_ref
        begin, size = parts[piece - 1]
        return shard_ref.at[pl.ds(begin, size)]

    started = []

    def push(piece, column, row, held, peers):
        for peer in peers:
            copy = pltpu.make_async_remote_copy(
                src_ref=held,
                dst_ref=place(piece, column, row),
                send_sem=send_sem.at[len(started)],
                recv_sem=recv_sem.at[piece, column, row],
                device_id=peer,
                device_id_type=MESH,
            )
            copy.start()
            started.append(copy)

    def arrived(piece, column, row):
        block = place(piece, column, row)
        pltpu.make_async_remote_copy(
            src_ref=block,
            dst_ref=block,
            send_sem=send_sem.at[0],
            recv_sem=recv_sem.at[piece, column, row],
            device_id=partner,
            device_id_type=MESH,
        ).wait_recv()
        return block

    def dims(piece):
        if piece == 2:
            return (along_y, y_ids, True), (along_x, x_ids, False)
        return (along_x, x_ids, False), (along_y, y_ids, True)

    kept = []
    for piece in range(3):
        copy = pltpu.make_async_copy(source(piece), place(piece, me_dp, me_fsdp), own_sem.at[piece])
        copy.start()
        kept.append(copy)
        first, second = dims(piece)
        push(piece, me_dp, me_fsdp, source(piece), z_ids + first[1] + second[1] + [partner])
    for other in along_z:
        for piece in range(3):
            first, second = dims(piece)
            row = other * 2 + core
            push(piece, me_dp, row, arrived(piece, me_dp, row), first[1] + second[1] + [partner])
    all_z = [z] + along_z
    for other in all_z:
        for piece in range(3):
            first, second = dims(piece)
            row = other * 2 + core
            for place_one in first[0]:
                column = place_one * low + x if first[2] else y * low + place_one
                push(piece, column, row, arrived(piece, column, row), second[1] + [partner])
    for other in all_z:
        for piece in range(3):
            first, second = dims(piece)
            own_first = y if first[2] else x
            row = other * 2 + core
            for place_two in second[0]:
                for place_one in [own_first] + first[0]:
                    column = (
                        place_one * low + place_two if first[2] else place_two * low + place_one
                    )
                    push(piece, column, row, arrived(piece, column, row), [partner])
    for other in all_z:
        for piece in range(3):
            for place_y in [y] + along_y:
                for place_x in [x] + along_x:
                    arrived(piece, place_y * low + place_x, other * 2 + 1 - core)
    for copy in kept:
        copy.wait()
    for copy in started:
        copy.wait_send()


def gather_all(shard, vec_shard, dp_size, fsdp_size):
    cut = shard.shape[0] // 2 // 16 * 16
    high, low = split_two(dp_size)
    depth = fsdp_size // 2
    sends = 0
    for first, second in ((low, high), (low, high), (high, low)):
        sends += (depth - 1) + depth * (first - 1) + depth * first * (second - 1)
        sends += depth * first * second
    return pl.pallas_call(
        partial(gather_kernel, dp_size, fsdp_size, cut),
        out_shape=(
            jax.ShapeDtypeStruct((fsdp_size, dp_size) + shard.shape, shard.dtype),
            jax.ShapeDtypeStruct((dp_size, fsdp_size) + vec_shard.shape, vec_shard.dtype),
        ),
        in_specs=[pl.BlockSpec(memory_space=pltpu.VMEM)] * 2,
        out_specs=(pl.BlockSpec(memory_space=pltpu.VMEM),) * 2,
        scratch_shapes=[
            pltpu.SemaphoreType.DMA((sends,)),
            pltpu.SemaphoreType.DMA((3, dp_size, fsdp_size)),
            pltpu.SemaphoreType.DMA((3,)),
        ],
        compiler_params=pltpu.CompilerParams(
            collective_id=0, has_side_effects=True, vmem_limit_bytes=20 << 20
        ),
        name="gather_all",
    )(shard, vec_shard)


def reduce_kernel(
    dp_size,
    fsdp_size,
    big_ref,
    small_ref,
    big_out_ref,
    small_out_ref,
    big_near,
    small_near,
    big_sum,
    small_sum,
    big_dp,
    small_dp,
    big_part,
    small_part,
    big_z,
    small_z,
    big_end,
    small_end,
    send_sem,
    near_sem,
    dp_sem,
    z_sem,
    big_sem,
    small_sem,
    own_sem,
):
    depth = fsdp_size // 2
    me_dp, me_fsdp = lax.axis_index("dp"), lax.axis_index("fsdp")
    z, core = me_fsdp // 2, lax.rem(me_fsdp, 2)
    along_dp = [lax.rem(me_dp + i, dp_size) for i in range(1, dp_size)]
    along_z = [lax.rem(z + i, depth) for i in range(1, depth)]
    partner = (me_dp, z * 2 + 1 - core)
    dp_ids = [(other, me_fsdp) for other in along_dp]
    z_ids = [(me_dp, other * 2 + core) for other in along_z]
    meet([partner] + dp_ids + z_ids)
    started = []

    def push(held, target, semaphore, peer):
        copy = pltpu.make_async_remote_copy(
            src_ref=held,
            dst_ref=target,
            send_sem=send_sem.at[len(started)],
            recv_sem=semaphore,
            device_id=peer,
            device_id_type=MESH,
        )
        copy.start()
        started.append(copy)

    def arrived(block, semaphore):
        pltpu.make_async_remote_copy(
            src_ref=block,
            dst_ref=block,
            send_sem=send_sem.at[0],
            recv_sem=semaphore,
            device_id=partner,
            device_id_type=MESH,
        ).wait_recv()

    def wide(block):
        return block.astype(jnp.float32)

    for other in along_dp + [me_dp]:
        push(big_ref.at[1 - core, other], big_near.at[other], near_sem.at[0, other], partner)
        push(small_ref.at[1 - core, other], small_near.at[other], near_sem.at[1, other], partner)
    for other, peer in zip(along_dp, dp_ids):
        arrived(big_near.at[other], near_sem.at[0, other])
        arrived(small_near.at[other], near_sem.at[1, other])
        for level in range(depth):
            big_sum[other, level] = (
                wide(big_ref[core, other, level]) + wide(big_near[other, level])
            ).astype(big_sum.dtype)
            small_sum[other, level] = (
                wide(small_ref[core, other, level]) + wide(small_near[other, level])
            ).astype(small_sum.dtype)
        for level in range(depth):
            push(
                big_sum.at[other, level],
                big_dp.at[me_dp, level],
                dp_sem.at[0, me_dp, level],
                peer,
            )
            push(
                small_sum.at[other, level],
                small_dp.at[me_dp, level],
                dp_sem.at[1, me_dp, level],
                peer,
            )
    arrived(big_near.at[me_dp], near_sem.at[0, me_dp])
    arrived(small_near.at[me_dp], near_sem.at[1, me_dp])

    def over_dp(level):
        big = wide(big_ref[core, me_dp, level]) + wide(big_near[me_dp, level])
        small = wide(small_ref[core, me_dp, level]) + wide(small_near[me_dp, level])
        for other in along_dp:
            arrived(big_dp.at[other, level], dp_sem.at[0, other, level])
            arrived(small_dp.at[other, level], dp_sem.at[1, other, level])
            big = big + wide(big_dp[other, level])
            small = small + wide(small_dp[other, level])
        return big, small

    for level, peer in zip(along_z, z_ids):
        big, small = over_dp(level)
        big_part[level] = big.astype(big_part.dtype)
        small_part[level] = small.astype(small_part.dtype)
        push(big_part.at[level], big_z.at[z], z_sem.at[0, z], peer)
        push(small_part.at[level], small_z.at[z], z_sem.at[1, z], peer)
    big, small = over_dp(z)
    for level in along_z:
        arrived(small_z.at[level], z_sem.at[1, level])
        small = small + wide(small_z[level])
    small_end[...] = small.astype(small_end.dtype)
    for peer in z_ids + dp_ids + [partner]:
        push(small_end, small_out_ref.at[core, me_dp, z], small_sem.at[core, me_dp, z], peer)
    for level in along_z:
        arrived(big_z.at[level], z_sem.at[0, level])
        big = big + wide(big_z[level])
    big_end[...] = big.astype(big_end.dtype)
    for peer in dp_ids:
        push(big_end, big_out_ref.at[me_dp], big_sem.at[me_dp], peer)
    kept = [
        pltpu.make_async_copy(small_end, small_out_ref.at[core, me_dp, z], own_sem.at[0]),
        pltpu.make_async_copy(big_end, big_out_ref.at[me_dp], own_sem.at[1]),
    ]
    for copy in kept:
        copy.start()
    for level in along_z:
        block = small_out_ref.at[core, me_dp, level]
        arrived(block, small_sem.at[core, me_dp, level])
        for peer in dp_ids + [partner]:
            push(block, block, small_sem.at[core, me_dp, level], peer)
    for level in [z] + along_z:
        for other in along_dp:
            block = small_out_ref.at[core, other, level]
            arrived(block, small_sem.at[core, other, level])
            push(block, block, small_sem.at[core, other, level], partner)
    for other in along_dp:
        arrived(big_out_ref.at[other], big_sem.at[other])
    for level in [z] + along_z:
        for other in [me_dp] + along_dp:
            arrived(
                small_out_ref.at[1 - core, other, level], small_sem.at[1 - core, other, level]
            )
    for copy in kept:
        copy.wait()
    for copy in started:
        copy.wait_send()


def reduce_all(big, small, dp_size, fsdp_size):
    depth = fsdp_size // 2
    sends = 2 * dp_size + 2 * (dp_size - 1) * depth + 2 * (depth - 1)
    sends += (depth - 1) + dp_size + (dp_size - 1)
    sends += (depth - 1) * dp_size + depth * (dp_size - 1)
    shapes = (big.shape[3:], small.shape[3:])
    low = big.dtype
    scratch = []
    for lead in ((dp_size, depth), (dp_size, depth), (dp_size, depth), (depth,), (depth,), ()):
        scratch += [pltpu.VMEM(lead + shape, low) for shape in shapes]
    return pl.pallas_call(
        partial(reduce_kernel, dp_size, fsdp_size),
        out_shape=(
            jax.ShapeDtypeStruct((dp_size,) + shapes[0], low),
            jax.ShapeDtypeStruct(small.shape, low),
        ),
        in_specs=[pl.BlockSpec(memory_space=pltpu.VMEM)] * 2,
        out_specs=(pl.BlockSpec(memory_space=pltpu.VMEM),) * 2,
        scratch_shapes=scratch
        + [
            pltpu.SemaphoreType.DMA((sends,)),
            pltpu.SemaphoreType.DMA((2, dp_size)),
            pltpu.SemaphoreType.DMA((2, dp_size, depth)),
            pltpu.SemaphoreType.DMA((2, depth)),
            pltpu.SemaphoreType.DMA((dp_size,)),
            pltpu.SemaphoreType.DMA((2, dp_size, depth)),
            pltpu.SemaphoreType.DMA((2,)),
        ],
        compiler_params=pltpu.CompilerParams(
            collective_id=1, has_side_effects=True, vmem_limit_bytes=20 << 20
        ),
        name="reduce_all",
    )(big, small)


def scalar_kernel(
    dp_size, fsdp_size, part_ref, out_ref, row_slots, row_sum, dp_slots, send_sem, row_sem, dp_sem
):
    me_dp, me_fsdp = lax.axis_index("dp"), lax.axis_index("fsdp")
    along_dp = [lax.rem(me_dp + i, dp_size) for i in range(1, dp_size)]
    along_fsdp = [lax.rem(me_fsdp + i, fsdp_size) for i in range(1, fsdp_size)]
    meet([(me_dp, other) for other in along_fsdp] + [(other, me_fsdp) for other in along_dp])
    started = []

    def exchange(held, slots, semaphores, me, others, peers):
        for peer in peers:
            copy = pltpu.make_async_remote_copy(
                src_ref=held,
                dst_ref=slots.at[me],
                send_sem=send_sem.at[len(started)],
                recv_sem=semaphores.at[me],
                device_id=peer,
                device_id_type=MESH,
            )
            copy.start()
            started.append(copy)
        slots[me] = held[...]
        for other in others:
            pltpu.make_async_remote_copy(
                src_ref=held,
                dst_ref=slots.at[other],
                send_sem=send_sem.at[0],
                recv_sem=semaphores.at[other],
                device_id=peers[0],
                device_id_type=MESH,
            ).wait_recv()
        total = slots[0]
        for place in range(1, len(others) + 1):
            total = total + slots[place]
        return total

    row_sum[...] = exchange(
        part_ref, row_slots, row_sem, me_fsdp, along_fsdp, [(me_dp, other) for other in along_fsdp]
    )
    out_ref[...] = exchange(
        row_sum, dp_slots, dp_sem, me_dp, along_dp, [(other, me_fsdp) for other in along_dp]
    )
    for copy in started:
        copy.wait_send()


def scalar_sums(tile, dp_size, fsdp_size):
    return pl.pallas_call(
        partial(scalar_kernel, dp_size, fsdp_size),
        out_shape=jax.ShapeDtypeStruct((8, 128), jnp.float32),
        in_specs=[pl.BlockSpec(memory_space=pltpu.VMEM)],
        out_specs=pl.BlockSpec(memory_space=pltpu.VMEM),
        scratch_shapes=[
            pltpu.VMEM((fsdp_size, 8, 128), jnp.float32),
            pltpu.VMEM((8, 128), jnp.float32),
            pltpu.VMEM((dp_size, 8, 128), jnp.float32),
            pltpu.SemaphoreType.DMA((fsdp_size + dp_size,)),
            pltpu.SemaphoreType.DMA((fsdp_size,)),
            pltpu.SemaphoreType.DMA((dp_size,)),
        ],
        compiler_params=pltpu.CompilerParams(collective_id=2, has_side_effects=True, vmem_limit_bytes=4 << 20),
        name="scalar_sums",
    )(tile)


def three_parts(values):
    high = values.astype(jnp.bfloat16)
    rest = values - high.astype(jnp.float32)
    middle = rest.astype(jnp.bfloat16)
    return high, middle, (rest - middle.astype(jnp.float32)).astype(jnp.bfloat16)


def product(left, right, left_axis, right_axis):
    return lax.dot_general(
        left,
        right,
        (((left_axis,), (right_axis,)), ((), ())),
        preferred_element_type=jnp.float32,
    )


def local_step_kernel(
    chunk,
    embed_ref,
    head_ref,
    rows_ref,
    onehot_ref,
    target_ref,
    weight_ref,
    big_ref,
    taps_ref,
    wide_ref,
    loss_ref,
    inner_ref,
    first_ref,
    placed_ref,
    spread,
    tap_table,
    kept_third,
    kept_grad,
    sums,
):
    fsdp_size, inner, packed = weight_ref.shape
    width = embed_ref.shape[1]
    own = width // fsdp_size
    own_conv = packed - 2 * own
    slots = onehot_ref.shape[0]
    gain_one, bias_one = rows_ref[0:1, :], rows_ref[1:2, :]
    first_low = norm_gelu(embed_ref[...], gain_one, bias_one).astype(jnp.bfloat16)
    pre_inner = jnp.broadcast_to(rows_ref[6:7, :inner], (TABLE, inner))
    for row in range(fsdp_size):
        block = first_low[:, row * own : (row + 1) * own]
        first_ref[row] = block
        pre_inner = pre_inner + product(
            block, weight_ref[row, :, own_conv : own_conv + own], 1, 1
        )
    inner_ref[...] = pre_inner
    second_low = norm_gelu(pre_inner, rows_ref[5:6, :inner], rows_ref[5:6, inner:]).astype(
        jnp.bfloat16
    )
    spread[...] = jnp.zeros_like(spread)
    for tap in range(CONV_TAPS):
        spread[tap * TABLE : (tap + 1) * TABLE, tap * inner : (tap + 1) * inner] = second_low
    total = jnp.zeros((CONV_TAPS * TABLE, inner), jnp.float32)
    for row in range(fsdp_size):
        block = spread[:, row * own_conv : (row + 1) * own_conv]
        placed_ref[row] = block
        total = total + product(block, weight_ref[row, :, :own_conv], 1, 1)
    tap_table[...] = jnp.concatenate(three_parts(total), axis=1)
    sums[...] = jnp.zeros_like(sums)
    taps_ref[...] = jnp.zeros_like(taps_ref)
    wide_ref[...] = jnp.zeros_like(wide_ref)
    embed_low = embed_ref[...].astype(jnp.bfloat16)
    head = head_ref[...]
    gain_four, bias_four = rows_ref[3:4, :], rows_ref[4:5, :]

    def one_chunk(index, carry):
        here = pl.ds(pl.multiple_of(index * chunk, chunk), chunk)
        onehot = onehot_ref[here, :]
        centre = onehot[:, CONV_TAPS // 2 * TABLE : (CONV_TAPS // 2 + 1) * TABLE]
        parts = product(onehot, tap_table[...], 1, 0)
        conv_input = (
            parts[:, :inner]
            + parts[:, inner : 2 * inner]
            + parts[:, 2 * inner :]
            + rows_ref[6:7, inner:]
        )
        third_act, third_back = jax.vjp(
            norm_gelu, conv_input, rows_ref[7:8, :inner], rows_ref[7:8, inner:]
        )
        third_low = third_act.astype(jnp.bfloat16)
        kept_third[here, :] = third_low
        branch = jnp.concatenate(
            [
                product(third_low, weight_ref[row, :, own_conv + own :], 1, 0)
                for row in range(fsdp_size)
            ],
            axis=1,
        )
        summed = product(centre, embed_low, 1, 0) + branch + rows_ref[2:3, :]
        final, final_back = jax.vjp(layer_norm, summed, gain_four, bias_four)
        picked = final.astype(jnp.bfloat16)
        logits = product(picked, head, 1, 1)
        lanes = lax.broadcasted_iota(jnp.int32, logits.shape, 1)
        logits = jnp.where(lanes < VOCAB, logits, -1e30)
        target = target_ref[here, :]
        valid = target >= 0
        highest = jnp.max(logits, axis=1, keepdims=True)
        powers = jnp.exp(logits - highest)
        power_sum = jnp.sum(powers, axis=1, keepdims=True)
        hits = lanes == target
        chosen = jnp.sum(jnp.where(hits, logits, 0.0), axis=1, keepdims=True)
        losses = jnp.where(valid, jnp.log(power_sum) + highest - chosen, 0.0)
        logit_grad = jnp.where(valid, powers / power_sum - hits.astype(jnp.float32), 0.0).astype(
            jnp.bfloat16
        )
        picked_grad = product(logit_grad, head, 1, 0)
        sum_grad, gain_grad, bias_grad = final_back(picked_grad)
        branch_low = sum_grad.astype(jnp.bfloat16)
        kept_grad[here, :] = branch_low
        third_grad = jnp.zeros((chunk, inner), jnp.float32)
        for row in range(fsdp_size):
            third_grad = third_grad + product(
                branch_low[:, row * own : (row + 1) * own],
                weight_ref[row, :, own_conv + own :],
                1,
                1,
            )
        conv_pre, gain_three, bias_three = third_back(third_grad)
        taps_ref[...] += product(onehot, conv_pre.astype(jnp.bfloat16), 0, 0)
        high, middle, low = three_parts(sum_grad)
        wide_ref[0:TABLE, :] += (
            product(centre, high, 0, 0) + product(centre, middle, 0, 0) + product(centre, low, 0, 0)
        )
        wide_ref[TABLE : 2 * TABLE, :] += product(logit_grad, picked, 0, 0)
        wide_ref[2 * TABLE : 2 * TABLE + 1, :] += jnp.sum(
            branch_low.astype(jnp.float32), axis=0, keepdims=True
        )
        wide_ref[2 * TABLE + 1 : 2 * TABLE + 2, :] += gain_grad
        wide_ref[2 * TABLE + 2 : 2 * TABLE + 3, :] += bias_grad
        wide_ref[2 * TABLE + 3 : 2 * TABLE + 4, :inner] += gain_three
        wide_ref[2 * TABLE + 3 : 2 * TABLE + 4, inner:] += bias_three
        sums[0:1, :] += jnp.sum(jnp.broadcast_to(losses, (chunk, 128)), axis=0, keepdims=True)
        sums[1:2, :] += jnp.sum(
            jnp.broadcast_to(valid.astype(jnp.float32), (chunk, 128)), axis=0, keepdims=True
        )
        return carry

    lax.fori_loop(0, slots // chunk, one_chunk, 0)
    loss_ref[...] = sums[...]
    third_all = kept_third[...]

    for row in range(fsdp_size):
        big_ref[row] = product(
            kept_grad[:, row * own : (row + 1) * own], third_all, 0, 0
        ).astype(jnp.bfloat16)


def local_step(embed, head, rows, onehots, targets, weights):
    fsdp_size, inner, packed = weights.shape
    slots, width = onehots.shape[0], embed.shape[1]
    own = width // fsdp_size
    own_conv = packed - 2 * own
    shape = jax.ShapeDtypeStruct
    vmem = pl.BlockSpec(memory_space=pltpu.VMEM)
    return pl.pallas_call(
        partial(local_step_kernel, min(slots, 128)),
        out_shape=(
            shape((fsdp_size, own, inner), jnp.bfloat16),
            shape((CONV_TAPS * TABLE, inner), jnp.float32),
            shape((2 * TABLE + 8, width), jnp.float32),
            shape((8, 128), jnp.float32),
            shape((TABLE, inner), jnp.float32),
            shape((fsdp_size, TABLE, own), jnp.bfloat16),
            shape((fsdp_size, CONV_TAPS * TABLE, own_conv), jnp.bfloat16),
        ),
        in_specs=[vmem] * 6,
        out_specs=(vmem,) * 7,
        scratch_shapes=[
            pltpu.VMEM((CONV_TAPS * TABLE, CONV_TAPS * inner), jnp.bfloat16),
            pltpu.VMEM((CONV_TAPS * TABLE, 3 * inner), jnp.bfloat16),
            pltpu.VMEM((slots, inner), jnp.bfloat16),
            pltpu.VMEM((slots, width), jnp.bfloat16),
            pltpu.VMEM((8, 128), jnp.float32),
        ],
        compiler_params=pltpu.CompilerParams(vmem_limit_bytes=28 << 20),
        name="local_step",
    )(embed, head, rows, onehots, targets, weights)


def table_step_kernel(
    small_ref,
    embed_ref,
    rows_ref,
    weight_ref,
    inner_ref,
    first_ref,
    placed_ref,
    out_rows_ref,
    in_rows_ref,
    conv_rows_ref,
    vec_ref,
    square_ref,
):
    fsdp_size, inner, packed = weight_ref.shape
    width = embed_ref.shape[1]
    own = width // fsdp_size
    own_conv = packed - 2 * own
    me_dp, me_fsdp = lax.axis_index("dp"), lax.axis_index("fsdp")
    tap_rows = CONV_TAPS * TABLE
    wide_count = 2 * TABLE + 8
    small = small_ref[...].astype(jnp.float32)
    taps = jnp.concatenate(
        [small[at * tap_rows : (at + 1) * tap_rows] for at in range(inner // 128)], axis=1
    )
    begin = tap_rows * (inner // 128)
    wide = jnp.concatenate(
        [
            small[begin + at * wide_count : begin + (at + 1) * wide_count]
            for at in range(width // 128)
        ],
        axis=1,
    )
    conv_rows_ref[...] = product(placed_ref[me_fsdp], taps.astype(jnp.bfloat16), 0, 0)
    taps_low = taps.astype(jnp.bfloat16)
    columns = jnp.concatenate(
        [
            product(taps_low, weight_ref[row, :, :own_conv], 1, 0)
            for row in range(fsdp_size)
        ],
        axis=1,
    )
    second_grad = jnp.zeros((TABLE, inner), jnp.float32)
    for tap in range(CONV_TAPS):
        second_grad = second_grad + columns[
            tap * TABLE : (tap + 1) * TABLE, tap * inner : (tap + 1) * inner
        ]
    second_back = jax.vjp(
        norm_gelu, inner_ref[...], rows_ref[5:6, :inner], rows_ref[5:6, inner:]
    )[1]
    inner_pre, gain_two, bias_two = second_back(second_grad)
    high, middle, low = three_parts(inner_pre)
    first_own = first_ref[me_fsdp]
    in_rows_ref[...] = (
        product(first_own, high, 0, 0) + product(first_own, middle, 0, 0) + product(first_own, low, 0, 0)
    )
    stacked = jnp.concatenate([high, middle], axis=0)
    pieces = []
    for row in range(fsdp_size):
        piece = product(stacked, weight_ref[row, :, own_conv : own_conv + own], 1, 0)
        pieces.append(piece[:TABLE] + piece[TABLE:])
    first_back = jax.vjp(norm_gelu, embed_ref[...], rows_ref[0:1, :], rows_ref[1:2, :])[1]
    table_grad, gain_one, bias_one = first_back(jnp.concatenate(pieces, axis=1))
    centre = CONV_TAPS // 2 * TABLE
    vec_ref[0:TABLE, :] = table_grad + wide[0:TABLE]
    vec_ref[TABLE : 2 * TABLE, :] = wide[TABLE : 2 * TABLE]
    vec_ref[2 * TABLE : 2 * TABLE + 1, :] = gain_one
    vec_ref[2 * TABLE + 1 : 2 * TABLE + 2, :] = bias_one
    vec_ref[2 * TABLE + 2 : 2 * TABLE + 5, :] = wide[2 * TABLE : 2 * TABLE + 3]
    vec_ref[2 * TABLE + 5 : 2 * TABLE + 6, :inner] = gain_two
    vec_ref[2 * TABLE + 5 : 2 * TABLE + 6, inner:] = bias_two
    vec_ref[2 * TABLE + 6 : 2 * TABLE + 7, :inner] = jnp.sum(inner_pre, axis=0, keepdims=True)
    vec_ref[2 * TABLE + 6 : 2 * TABLE + 7, inner:] = jnp.sum(
        taps[centre : centre + TABLE], axis=0, keepdims=True
    )
    vec_ref[2 * TABLE + 7 : 2 * TABLE + 8, :] = wide[2 * TABLE + 3 : 2 * TABLE + 4]

    def squares(values, group, block):
        lanes = lax.broadcasted_iota(jnp.int32, values.shape, 1)
        mine = (lanes >= group * block) & (lanes < (group + 1) * block)
        kept = jnp.where(mine, values, 0.0)
        rows = jnp.sum(kept * kept, axis=0, keepdims=True)
        return jnp.sum(rows, axis=1, keepdims=True)

    groups = lax.axis_size("dp")
    block = inner // groups
    total = squares(in_rows_ref[...], me_dp, block)
    total = total + squares(conv_rows_ref[...], me_dp, block)
    total = total + squares(out_rows_ref[...].astype(jnp.float32), me_dp, block)
    vec_block = width // (groups * fsdp_size)
    total = total + squares(vec_ref[...], me_dp * fsdp_size + me_fsdp, vec_block)
    square_ref[...] = jnp.broadcast_to(total, square_ref.shape)


def table_step(small, embed, rows, weights, pre_inner, first_low, placed, out_rows):
    fsdp_size, inner, packed = weights.shape
    width = embed.shape[1]
    own = width // fsdp_size
    shape = jax.ShapeDtypeStruct
    vmem = pl.BlockSpec(memory_space=pltpu.VMEM)
    return pl.pallas_call(
        table_step_kernel,
        out_shape=(
            shape((own, inner), jnp.float32),
            shape((packed - 2 * own, inner), jnp.float32),
            shape((2 * TABLE + 8, width), jnp.float32),
            shape((8, 128), jnp.float32),
        ),
        in_specs=[vmem] * 8,
        out_specs=(vmem,) * 4,
        compiler_params=pltpu.CompilerParams(vmem_limit_bytes=28 << 20),
        name="table_step",
    )(small, embed, rows, weights, pre_inner, first_low, placed, out_rows)


def precise(left, right, left_axis, right_axis):
    return lax.dot_general(
        left,
        right,
        (((left_axis,), (right_axis,)), ((), ())),
        precision=highest_precision,
        preferred_element_type=jnp.float32,
    )


def update_kernel(index, transposed, *refs):
    (
        flag_ref,
        step_ref,
        sums_ref,
        grad_ref,
        base_ref,
        master_ref,
        moment_ref,
        square_ref,
        master_out,
        copy_out,
        moment_out,
        square_out,
        rotated,
    ) = refs
    count = sums_ref[2:3, 0:1]
    grad_norm = jnp.sqrt(sums_ref[0:1, 0:1]) / count
    factor = jnp.minimum(1.0, clip_limit / grad_norm) / count
    first_correction, second_correction = corrections(step_ref[0])
    turned = flag_ref[index] == 1

    @pl.when(turned)
    def _():
        rotated[...] = precise(grad_ref[...].astype(jnp.float32), base_ref[0], 1, 0)

    @pl.when(jnp.logical_not(turned))
    def _():
        rotated[...] = grad_ref[...].astype(jnp.float32)

    chunk = 40

    def one_chunk(step, carry):
        here = pl.ds(pl.multiple_of(step * chunk, 8), chunk)
        value = rotated[here, :] * factor
        moment = beta_one * moment_ref[here, :] + (1.0 - beta_one) * value
        square = beta_two * square_ref[here, :] + (1.0 - beta_two) * value * value
        moment_out[here, :] = moment
        square_out[here, :] = square
        rotated[here, :] = (
            moment / first_correction / (jnp.sqrt(square / second_correction) + epsilon)
        )
        return carry

    lax.fori_loop(0, rotated.shape[0] // chunk, one_chunk, 0)
    width = master_ref.shape[0] if transposed else master_ref.shape[1]
    start = lax.axis_index("dp") * width

    def finish(update):
        master = master_ref[...]
        master = master - rate_matrix * (update + decay_weight * master)
        master_out[...] = master
        copy_out[...] = master.astype(jnp.bfloat16)

    own_rows = pl.ds(pl.multiple_of(start, 8), width)

    @pl.when(turned)
    def _():
        if transposed:
            finish(precise(base_ref[0, own_rows, :], rotated[...], 1, 1))
        else:
            finish(precise(rotated[...], base_ref[0, own_rows, :], 1, 1))

    @pl.when(jnp.logical_not(turned))
    def _():
        inner = rotated.shape[1]
        rows = lax.broadcasted_iota(jnp.int32, (width, inner), 0) + start
        picks = (rows == lax.broadcasted_iota(jnp.int32, (width, inner), 1)).astype(jnp.float32)
        if transposed:
            finish(precise(picks, rotated[...], 1, 1))
        else:
            finish(precise(rotated[...], picks, 1, 1))


def corrections(step):
    value = jnp.full((1, 1), step.astype(jnp.float32))
    return 1.0 - jnp.exp(value * math.log(beta_one)), 1.0 - jnp.exp(value * math.log(beta_two))


def matrix_update(index, transposed, flags, step, sums, gradient, bases, master, moment, square):
    inner = moment.shape[1]
    shape = jax.ShapeDtypeStruct
    vmem = pl.BlockSpec(memory_space=pltpu.VMEM)
    smem = pl.BlockSpec(memory_space=pltpu.SMEM)
    return pl.pallas_call(
        partial(update_kernel, index, transposed),
        grid=(1,),
        out_shape=(
            shape(master.shape, jnp.float32),
            shape(master.shape, jnp.bfloat16),
            shape(moment.shape, jnp.float32),
            shape(moment.shape, jnp.float32),
        ),
        in_specs=[smem, smem, vmem, vmem]
        + [pl.BlockSpec((1, inner, inner), lambda at: (index, 0, 0))]
        + [vmem] * 3,
        out_specs=(vmem,) * 4,
        scratch_shapes=[pltpu.VMEM(moment.shape, jnp.float32)],
        compiler_params=pltpu.CompilerParams(vmem_limit_bytes=28 << 20),
        name="update_%d" % index,
    )(flags, step, sums, gradient, bases, master, moment, square)


def adam_vectors(gradient, master, moment, square, first_correction, second_correction):
    decay_rows = jnp.where(
        jnp.arange(master.shape[0], dtype=jnp.int32)[:, None] < 2 * VOCAB, decay_weight, 0.0
    )
    moment_new = beta_one * moment + (1.0 - beta_one) * gradient
    square_new = beta_two * square + (1.0 - beta_two) * gradient * gradient
    step_ratio = (
        moment_new / first_correction / (jnp.sqrt(square_new / second_correction) + epsilon)
    )
    master_new = master - rate_vector * (step_ratio + decay_rows * master)
    return (master_new, master_new.astype(jnp.bfloat16), moment_new, square_new)


def local(
    input_tokens,
    item_numbers,
    loss_positions,
    target_tokens,
    input_projection,
    dilated_conv,
    output_projection,
    vectors,
    input_first_moment,
    input_second_moment,
    conv_first_moment,
    conv_second_moment,
    output_first_moment,
    output_second_moment,
    vector_first_moment,
    vector_second_moment,
    bases,
    eigenbasis_flags,
    optimizer_step,
):
    groups, col_index = lax.axis_size("dp"), lax.axis_index("dp")
    rows, row_index = lax.axis_size("fsdp"), lax.axis_index("fsdp")
    own_conv, own_in = dilated_conv.shape[0], input_projection.shape[0]
    shard = jnp.concatenate([dilated_conv, input_projection, output_projection], axis=0)
    all_weights, all_vectors = gather_all(
        shard.astype(jnp.bfloat16).T,
        lax.reduce_precision(vectors, 8, 7).T,
        groups,
        rows,
    )

    width = own_in * rows
    inner = groups * input_projection.shape[1]
    start = 2 * VOCAB
    weights = all_weights.reshape(rows, inner, -1)
    table = all_vectors.reshape(width, -1).T
    spare = jnp.zeros((TABLE - VOCAB, width), jnp.float32)
    embedded = jnp.concatenate([table[:VOCAB], spare], axis=0)
    head = jnp.concatenate([table[VOCAB:start], spare], axis=0).astype(jnp.bfloat16)
    norm_rows = table[start:]
    onehots = tap_onehots(input_tokens, item_numbers, loss_positions)
    targets = jnp.where(loss_positions >= 0, target_tokens, -1).reshape(-1, 1)
    out_grad, tap_grads, wide_rows, loss_tile, pre_inner, first_low, placed = local_step(
        embedded, head, norm_rows, onehots.astype(jnp.bfloat16), targets, weights
    )
    depth = rows // 2
    big = out_grad.reshape(depth, 2, groups, -1, inner)
    flat = jnp.concatenate(
        [tap_grads[:, at : at + 128] for at in range(0, inner, 128)]
        + [wide_rows[:, at : at + 128] for at in range(0, width, 128)],
        axis=0,
    )
    piece = -(-flat.shape[0] // (groups * rows * 16)) * 16
    padding = jnp.zeros((piece * groups * rows - flat.shape[0], 128), jnp.float32)
    small = jnp.concatenate([flat, padding], axis=0).astype(jnp.bfloat16)
    out_rows, small = reduce_all(
        big.transpose(1, 2, 0, 3, 4), small.reshape(2, groups, depth, piece, 128), groups, rows
    )
    out_rows = out_rows.reshape(-1, inner)
    in_rows, conv_rows, vec_sum, square_tile = table_step(
        small.reshape(-1, 128), embedded, norm_rows, weights, pre_inner, first_low, placed, out_rows
    )
    vec_sum = jnp.concatenate(
        [vec_sum[:VOCAB], vec_sum[TABLE : TABLE + VOCAB], vec_sum[2 * TABLE :]], axis=0
    )
    own = width // (groups * rows)
    vec_own = lax.dynamic_slice_in_dim(vec_sum, (col_index * rows + row_index) * own, own, 1)

    tile = jnp.concatenate([square_tile[:1], loss_tile[:7]], axis=0)
    sums = scalar_sums(tile, groups, rows)
    slot_count = sums[2, 0]
    grad_norm = jnp.sqrt(sums[0, 0]) / slot_count
    factor = jnp.minimum(1.0, clip_limit / grad_norm) / slot_count
    first_correction, second_correction = corrections(optimizer_step[0])
    first_correction, second_correction = first_correction[0, 0], second_correction[0, 0]
    master_in, copy_in, moment_in, square_in = matrix_update(
        0,
        False,
        eigenbasis_flags,
        optimizer_step,
        sums,
        in_rows,
        bases,
        input_projection,
        input_first_moment,
        input_second_moment,
    )
    updated_conv, conv_bfloat_copy, updated_conv_moment, updated_conv_square = matrix_update(
        1,
        True,
        eigenbasis_flags,
        optimizer_step,
        sums,
        conv_rows,
        bases,
        dilated_conv.T,
        conv_first_moment,
        conv_second_moment,
    )
    updated_conv, conv_bfloat_copy = updated_conv.T, conv_bfloat_copy.T
    master_out, copy_out, moment_out, square_out = matrix_update(
        2,
        False,
        eigenbasis_flags,
        optimizer_step,
        sums,
        out_rows,
        bases,
        output_projection,
        output_first_moment,
        output_second_moment,
    )
    master_vec, copy_vec, moment_vec, square_vec = adam_vectors(
        vec_own * factor,
        vectors,
        vector_first_moment,
        vector_second_moment,
        first_correction,
        second_correction,
    )
    return (
        sums[1, 0] / slot_count,
        grad_norm,
        master_in,
        copy_in,
        moment_in,
        square_in,
        updated_conv,
        conv_bfloat_copy,
        updated_conv_moment,
        updated_conv_square,
        master_out,
        copy_out,
        moment_out,
        square_out,
        master_vec,
        copy_vec,
        moment_vec,
        square_vec,
    )


def solution(mesh):
    placed = (
        P(None, ("dp", "fsdp")),
        P(None, ("dp", "fsdp")),
        P(None, ("dp", "fsdp")),
        P(None, ("dp", "fsdp")),
        P("fsdp", "dp"),
        P("fsdp", "dp"),
        P("fsdp", "dp"),
        P(None, ("dp", "fsdp")),
        P("fsdp", None),
        P("fsdp", None),
        P("fsdp", None),
        P("fsdp", None),
        P("fsdp", None),
        P("fsdp", None),
        P(None, ("dp", "fsdp")),
        P(None, ("dp", "fsdp")),
        P(),
        P(),
        P(),
    )
    return jax.shard_map(
        local,
        mesh=mesh,
        in_specs=placed,
        out_specs=(
            P(),
            P(),
            P("fsdp", "dp"),
            P("fsdp", "dp"),
            P("fsdp", None),
            P("fsdp", None),
            P("fsdp", "dp"),
            P("fsdp", "dp"),
            P("fsdp", None),
            P("fsdp", None),
            P("fsdp", "dp"),
            P("fsdp", "dp"),
            P("fsdp", None),
            P("fsdp", None),
            P(None, ("dp", "fsdp")),
            P(None, ("dp", "fsdp")),
            P(None, ("dp", "fsdp")),
            P(None, ("dp", "fsdp")),
        ),
        check_vma=False,
    )
```
